128 devices in a mesh: dp: 1, tp: 2 (over core), sp: 64 (over z, y, x).
Axes of the slice: x: 4, y: 4, z: 4, core: 2. Of those that a mesh axis runs over, the one named last changes fastest.
Arguments:
- hidden: bfloat16 [64, 8192], P('dp')
- lengths: int32 [64], P('dp')
- k_cache: bfloat16 [64, 1024, 8, 128], P('dp', 'sp', 'tp')
- v_cache: bfloat16 [64, 1024, 8, 128], P('dp', 'sp', 'tp')
- norm_gain: bfloat16 [8192], replicated
- w_query: bfloat16 [8192, 8192], P(None, 'tp')
- w_key: bfloat16 [8192, 1024], P(None, 'tp')
- w_value: bfloat16 [8192, 1024], P(None, 'tp')
- w_out: bfloat16 [8192, 8192], P('tp')
Outputs:
- output 1: bfloat16 [64, 8192], P('dp')
- output 2: bfloat16 [64, 1024, 8, 128], P('dp', 'sp', 'tp')
- output 3: bfloat16 [64, 1024, 8, 128], P('dp', 'sp', 'tp')
All inputs are finite; a program needn't handle non-finite values.
Results may differ from the reference program's by a relative error of at most 0.00421083.
Values sent between devices are 32-bit elements.
A program may use at most 1 GiB of HBM per device.

```python
import jax
import jax.numpy as jnp
from jax import lax

D_MODEL = 8192
HEADS = 64
KV_HEADS = 8
HEAD_DIM = 128
BATCH = 64
SEQ_LEN = 1024

GROUP_SIZE = HEADS // KV_HEADS
SCALE = HEAD_DIM ** -0.5
EPS = 1e-6
NEG_BIG = -1e30


def setup_inputs(seed: int = 0, part: int = 0) -> dict:
    part_keys = jax.random.split(jax.random.fold_in(jax.random.key(seed), part), 4)
    shared_keys = jax.random.split(jax.random.key(seed + 1), 5)
    cache_shape = (BATCH, SEQ_LEN, KV_HEADS, HEAD_DIM)
    hidden = jax.random.normal(part_keys[0], (BATCH, D_MODEL), jnp.float32)
    lengths = jax.random.randint(part_keys[1], (BATCH,), 0, SEQ_LEN, jnp.int32)
    lengths = lengths.at[0].set(SEQ_LEN - 1)
    k_cache = jax.random.normal(part_keys[2], cache_shape, jnp.float32)
    steps = jax.random.normal(part_keys[3], cache_shape, jnp.float32)
    v_cache = jnp.cumsum(steps, axis=1) * (2.0 / SEQ_LEN) ** 0.5 + steps
    norm_gain = 1.0 + 0.5 * jax.random.normal(shared_keys[0], (D_MODEL,), jnp.float32)
    w_query = jax.random.normal(shared_keys[1], (D_MODEL, HEADS * HEAD_DIM), jnp.float32) * D_MODEL ** -0.5
    w_key = jax.random.normal(shared_keys[2], (D_MODEL, KV_HEADS * HEAD_DIM), jnp.float32) * D_MODEL ** -0.5
    w_value = jax.random.normal(shared_keys[3], (D_MODEL, KV_HEADS * HEAD_DIM), jnp.float32) * D_MODEL ** -0.5
    w_out = jax.random.normal(shared_keys[4], (HEADS * HEAD_DIM, D_MODEL), jnp.float32) * (HEADS * HEAD_DIM) ** -0.5
    return {
        'hidden': hidden.astype(jnp.bfloat16),
        'lengths': lengths,
        'k_cache': k_cache.astype(jnp.bfloat16),
        'v_cache': v_cache.astype(jnp.bfloat16),
        'norm_gain': norm_gain.astype(jnp.bfloat16),
        'w_query': w_query.astype(jnp.bfloat16),
        'w_key': w_key.astype(jnp.bfloat16),
        'w_value': w_value.astype(jnp.bfloat16),
        'w_out': w_out.astype(jnp.bfloat16),
    }


def reference(hidden, lengths, k_cache, v_cache, norm_gain, w_query, w_key, w_value, w_out):
    hid_f32 = hidden.astype(jnp.float32)
    inv_rms = lax.rsqrt(jnp.mean(hid_f32 * hid_f32, axis=-1, keepdims=True) + EPS)
    normed = (hid_f32 * inv_rms * norm_gain.astype(jnp.float32)).astype(jnp.bfloat16)
    query = jnp.dot(normed, w_query, preferred_element_type=jnp.float32).astype(jnp.bfloat16)
    new_key = jnp.dot(normed, w_key, preferred_element_type=jnp.float32).astype(jnp.bfloat16)
    new_value = jnp.dot(normed, w_value, preferred_element_type=jnp.float32).astype(jnp.bfloat16)
    positions = jnp.arange(SEQ_LEN)
    at_slot = (positions[None, :] == lengths[:, None])[:, :, None, None]
    k_new = jnp.where(at_slot, new_key.reshape(BATCH, 1, KV_HEADS, HEAD_DIM), k_cache)
    v_new = jnp.where(at_slot, new_value.reshape(BATCH, 1, KV_HEADS, HEAD_DIM), v_cache)
    query_groups = query.reshape(BATCH, KV_HEADS, GROUP_SIZE, HEAD_DIM)

    def one_sequence(item):
        q_seq, k_seq, v_seq, length = item
        scores = jnp.einsum('kgd,tkd->kgt', q_seq.astype(jnp.float32), k_seq.astype(jnp.float32)) * SCALE
        valid = positions <= length
        scores = jnp.where(valid, scores, NEG_BIG)
        peak = jnp.max(scores, axis=-1, keepdims=True)
        exp_vals = jnp.where(valid, jnp.exp(scores - peak), 0.0)
        denom_sum = jnp.sum(exp_vals, axis=-1, keepdims=True)
        weighted = jnp.einsum('kgt,tkd->kgd', exp_vals.astype(jnp.bfloat16).astype(jnp.float32), v_seq.astype(jnp.float32))
        return (weighted / denom_sum).astype(jnp.bfloat16)

    attn_out = lax.map(one_sequence, (query_groups, k_new, v_new, lengths))
    proj_sum = jnp.dot(attn_out.reshape(BATCH, HEADS * HEAD_DIM), w_out, preferred_element_type=jnp.float32)
    hidden_out = (hid_f32 + proj_sum).astype(jnp.bfloat16)
    return (hidden_out, k_new, v_new)
```

```python
import functools

import jax
import jax.numpy as jnp
from jax import lax
from jax.experimental import pallas as pl
from jax.experimental.pallas import tpu as pltpu
from jax.sharding import PartitionSpec as P

EPS = 1e-6
NEG_BIG = -1e30
MESH = pl.DeviceIdType.MESH
F32, BF16 = jnp.float32, jnp.bfloat16

BATCH, D_MODEL, HEAD_DIM = 64, 8192, 128
KV, HEADS, GROUP = 4, 32, 8
SEQ = 16
STRIDE = (1, 4, 16)
TILES = (5, 5, 6)
OFFS = (0, 40, 80)
SLOTS, NCHUNK, CW = 11, 16, 512
GROUPS = ((24, 2, 2, 2), (0, 3, 2, 0), (12, 3, 2, 1), (2, 3, 1, 0), (14, 3, 1, 1), (32, 1, 1, 2), (36, 1, 1, 2))
AXES = (0, 1, 2)
LINE = (0, 1, 2, 3)
NEAR, FAR = (1, 3, 2), (2, 1, 3)


def kernel(lens, hid_h, gain_h, kc_h, vc_h, wq_h, wk_h, wv_h, wo_h,
           out_h, ko_h, vo_h,
           hid, gain, normed, kc, vc, qf, posm, acc, sfull,
           st_a, ra0, ra1, ra2, rst_a,
           b0_, b1_, b2_, st_b, rb0, rb1, rb2, rst_b,
           rc0, rc1, rc2, rst_c,
           attn, lhs, pout, pin, wbuf,
           in_sem, w_sem, out_sem, kv_sem,
           q_send, q_recv, a_send, a_recv, b_send, b_recv, c_send, c_recv,
           gb_send, gb_recv, ga_send, ga_recv, t_send, t_recv):
    sp = lax.axis_index("sp")
    tp = lax.axis_index("tp")
    coord = [sp % 4, (sp // 4) % 4, sp // 16]
    ra, redb, rb, rc = (ra0, ra1, ra2), (b0_, b1_, b2_), (rb0, rb1, rb2), (rc0, rc1, rc2)

    def peer(axis, r):
        c = coord[axis]
        t = (c + r) % 4
        return sp + (t - c) * STRIDE[axis], t

    c_hid = pltpu.make_async_copy(hid_h, hid, in_sem.at[0])
    c_gain = pltpu.make_async_copy(gain_h, gain, in_sem.at[1])
    c_hid.start()
    c_gain.start()
    x, y, z = coord

    def wcol(slot, half, hbm, col, width, at, sem):
        return pltpu.make_async_copy(
            hbm.at[pl.ds(half * 4096, 4096), pl.ds(pl.multiple_of(col, 128), width)],
            wbuf.at[slot, :, pl.ds(half * 256 + at, width)], sem)

    wq_copies = []
    chunks = (
        ((wq_h, (24 + 2 * z) * 128, 256, 0),),
        ((wq_h, (3 * x) * 128, 256, 0),),
        ((wq_h, (12 + 3 * y) * 128, 256, 0),),
        ((wq_h, (3 * x + 2) * 128, 128, 0), (wq_h, (12 + 3 * y + 2) * 128, 128, 128)),
        ((wk_h, z * 128, 128, 0), (wv_h, z * 128, 128, 128)),
    )
    nsem = 2
    for s, parts in enumerate(chunks):
        cs = []
        for half in range(2):
            for (hbm, col, width, at) in parts:
                cs.append(wcol(s, half, hbm, col, width, at, in_sem.at[nsem]))
                nsem += 1
        for c in cs:
            c.start()
        wq_copies.append(cs)
    c_k = pltpu.make_async_copy(kc_h, kc, kv_sem.at[0])
    c_v = pltpu.make_async_copy(vc_h, vc, kv_sem.at[1])
    c_k.start()
    c_v.start()

    barrier = pltpu.get_barrier_semaphore()
    for axis in AXES:
        for r in NEAR:
            pl.semaphore_signal(barrier, inc=1, device_id={"sp": peer(axis, r)[0]}, device_id_type=MESH)
    pl.semaphore_signal(barrier, inc=1, device_id={"tp": 1 - tp}, device_id_type=MESH)

    c_hid.wait()
    c_gain.wait()
    ss = jnp.zeros((BATCH, 128), F32)
    for c in range(0, D_MODEL, 512):
        h = hid[:, c:c + 512].astype(F32)
        h = h * h
        ss = ss + ((h[:, 0:128] + h[:, 128:256]) + (h[:, 256:384] + h[:, 384:512]))
    inv = lax.rsqrt(jnp.sum(ss, axis=1, keepdims=True) * (1.0 / D_MODEL) + EPS)
    for c in range(0, D_MODEL, 512):
        h = hid[:, c:c + 512].astype(F32)
        normed[:, c:c + 512] = (h * inv * gain[:, c:c + 512].astype(F32)).astype(BF16)

    def q_copy(g, r, own=True):
        base, mult, count, axis = GROUPS[g]
        c = coord[axis] if own else (coord[axis] + 4 - r) % 4
        rows = pl.ds(pl.multiple_of((base + mult * c) * BATCH, BATCH), count * BATCH)
        return pltpu.make_async_remote_copy(
            src_ref=qf.at[rows], dst_ref=qf.at[rows],
            send_sem=q_send.at[g, r - 1], recv_sem=q_recv.at[g, r - 1],
            device_id={"sp": peer(axis, r)[0]}, device_id_type=MESH)

    def wo_copy(j, slot):
        return pltpu.make_async_copy(
            wo_h.at[:, pl.ds(pl.multiple_of(j * CW, CW), CW)], wbuf.at[slot], w_sem.at[slot])

    def put(g, k, val):
        base, mult, count, axis = GROUPS[g]
        rows = pl.ds(pl.multiple_of((base + mult * coord[axis] + k) * BATCH, BATCH), BATCH)
        qf[rows, :] = val.astype(BF16).astype(F32)

    plan = (((0, 0), (0, 1)), ((1, 0), (1, 1)), ((2, 0), (2, 1)), ((3, 0), (4, 0)), ((5, 0), (6, 0)))
    for s in range(5):
        for c in wq_copies[s]:
            c.wait()
        if s == 4:
            for j in range(6):
                wo_copy(j, 5 + j).start()
        res = (jnp.dot(normed[:, 0:4096], wbuf[s, :, 0:256], preferred_element_type=F32)
               + jnp.dot(normed[:, 4096:8192], wbuf[s, :, 256:512], preferred_element_type=F32))
        (g0, k0), (g1, k1) = plan[s]
        put(g0, k0, res[:, 0:128])
        put(g1, k1, res[:, 128:256])
        if s == 0:
            pl.semaphore_wait(barrier, 10)
        for g in sorted({g0, g1}):
            for r in FAR:
                q_copy(g, r).start()
    for j in range(6, 11):
        wo_copy(j, j - 6).start()

    row = lax.broadcasted_iota(jnp.int32, (64, 128), 0)
    col = lax.broadcasted_iota(jnp.int32, (64, 128), 1)
    own = (row // 32 == col // 64) & ((row % 32) // GROUP == col % KV)
    posm[...] = jnp.where(own, sp * SEQ + (col % 64) // KV, 1 << 30)

    c_k.wait()
    c_v.wait()
    for g in range(7):
        for r in NEAR:
            q_copy(g, r, False).wait_recv()

    scale = HEAD_DIM ** -0.5
    rpos = sp * SEQ + lax.broadcasted_iota(jnp.int32, (64, 128), 0) // KV
    lane = lax.broadcasted_iota(jnp.int32, (8, 128), 1)
    UN = 4

    def attn_body(i, carry):
        lens_, qs, ks, vs = [], [], [], []
        for u in range(UN):
            b = (i * UN + u) * 2
            l0, l1 = lens[b], lens[b + 1]
            lens_.append((l0, l1))
            q = jnp.concatenate([qf[pl.ds(b, 32, stride=64), :], qf[pl.ds(b + 1, 32, stride=64), :]], axis=0)
            qs.append(q.astype(BF16))
            for ref, base, dst in ((kc, 32, ks), (vc, 36, vs)):
                both = []
                for e, ln in ((0, l0), (1, l1)):
                    new = qf[pl.ds(base * 64 + b + e, 4, stride=64), :]
                    new8 = jnp.concatenate([new, new], axis=0)
                    new64 = jnp.concatenate([new8] * 8, axis=0)
                    old = ref[pl.ds(pl.multiple_of((b + e) * 64, 64), 64), :]
                    both.append(jnp.where(rpos == ln, new64, old.astype(F32)).astype(BF16))
                val = jnp.concatenate(both, axis=0)
                ref[pl.ds(pl.multiple_of(b * 64, 128), 128), :] = val
                dst.append(val)
        ss_ = [lax.dot_general(qs[u], ks[u], (((1,), (1,)), ((), ())), preferred_element_type=F32) for u in range(UN)]
        ps, sts = [], []
        for u in range(UN):
            l0, l1 = lens_[u]
            pm = posm[...]
            valid = jnp.concatenate([pm[0:32] <= l0, pm[32:64] <= l1], axis=0)
            s = jnp.where(valid, ss_[u] * scale, NEG_BIG)
            m = jnp.max(s, axis=1, keepdims=True)
            e = jnp.where(valid, jnp.exp(s - m), 0.0)
            l = jnp.sum(e, axis=1, keepdims=True)
            ps.append(e.astype(BF16))
            col2 = lax.broadcasted_iota(jnp.int32, (64, 128), 1)
            sts.append(jnp.where(col2 < 64, m, l))
        for u in range(UN):
            b = (i * UN + u) * 2
            o = jnp.dot(ps[u], vs[u], preferred_element_type=F32)
            acc[pl.ds(b, 32, stride=64), :] = o[0:32]
            acc[pl.ds(b + 1, 32, stride=64), :] = o[32:64]
            sfull[pl.ds(b, 32, stride=64), :] = sts[u][0:32]
            sfull[pl.ds(b + 1, 32, stride=64), :] = sts[u][32:64]
        return carry

    lax.fori_loop(0, BATCH // 2 // UN, attn_body, 0)

    c_ko = pltpu.make_async_copy(kc, ko_h, kv_sem.at[0])
    c_vo = pltpu.make_async_copy(vc, vo_h, kv_sem.at[1])
    c_ko.start()
    c_vo.start()

    lane64 = lane % 64
    for c in AXES:
        n = TILES[c]
        for a in LINE:
            st = jnp.zeros((8, 128), F32)
            for p in LINE:
                for v in range(n):
                    r0 = (4 * a + p) * 128 + OFFS[c] + 8 * v
                    st = jnp.where(lane64 == p * n + v, sfull[r0:r0 + 8, :], st)
            st_a[c, a] = st

    def remote(src, dst, ss_sem, rs_sem, dev):
        return pltpu.make_async_remote_copy(
            src_ref=src, dst_ref=dst, send_sem=ss_sem, recv_sem=rs_sem,
            device_id={"sp": dev}, device_id_type=MESH)

    def copies_a(c, r):
        n = TILES[c]
        dev, t = peer(c, r)
        out = [remote(st_a.at[c, t], rst_a.at[c, r - 1], a_send.at[c, r - 1, 4], a_recv.at[c, r - 1, 4], dev)]
        for p in LINE:
            src = acc.at[pl.ds(pl.multiple_of(t * 512 + (p * 128 + OFFS[c]), 8), 8 * n)]
            out.append(remote(src, ra[c].at[r - 1, p], a_send.at[c, r - 1, p], a_recv.at[c, r - 1, p], dev))
        return out

    def copies_b(c, r):
        dev, t = peer((c + 1) % 3, r)
        return [remote(redb[c].at[t], rb[c].at[r - 1], b_send.at[c, r - 1, 0], b_recv.at[c, r - 1, 0], dev),
                remote(st_b.at[c, t], rst_b.at[c, r - 1], b_send.at[c, r - 1, 1], b_recv.at[c, r - 1, 1], dev)]

    def copies_c(c, r, own):
        axis = (c + 2) % 3
        dev, t = peer(axis, r)
        at = coord[axis] if own else (coord[axis] + 4 - r) % 4
        return [remote(rc[c].at[at], rc[c].at[at], c_send.at[c, r - 1, 0], c_recv.at[c, r - 1, 0], dev),
                remote(rst_c.at[c, at], rst_c.at[c, at], c_send.at[c, r - 1, 1], c_recv.at[c, r - 1, 1], dev)]

    def copy_gb(c, r, own):
        axis = (c + 1) % 3
        dev, t = peer(axis, r)
        at = coord[axis] if own else (coord[axis] + 4 - r) % 4
        rows = pl.ds(pl.multiple_of((4 * coord[c] + at) * 128 + OFFS[c], 8), 8 * TILES[c])
        return remote(attn.at[rows], attn.at[rows], gb_send.at[c, r - 1], gb_recv.at[c, r - 1], dev)

    def copies_ga(c, r, own):
        dev, t = peer(c, r)
        at = coord[c] if own else (coord[c] + 4 - r) % 4
        out = []
        for p in LINE:
            rows = pl.ds(pl.multiple_of((4 * at + p) * 128 + OFFS[c], 8), 8 * TILES[c])
            out.append(remote(attn.at[rows], attn.at[rows], ga_send.at[c, r - 1, p], ga_recv.at[c, r - 1, p], dev))
        return out

    for r in FAR:
        for c in AXES:
            for cp in copies_a(c, r):
                cp.start()

    def weights(stats):
        top = functools.reduce(jnp.maximum, stats)
        ws = [jnp.exp(s - top) for s in stats]
        l = sum(pltpu.roll(w, 64, 1) * s for w, s in zip(ws, stats))
        return top, ws, l

    def bc(w, j):
        return jnp.broadcast_to(w[:, j:j + 1], (8, 128))

    for c in AXES:
        n = TILES[c]
        for r in NEAR:
            for cp in copies_a(c, r):
                cp.wait_recv()
        a = coord[c]
        stats = [st_a[c, a]] + [rst_a[c, r] for r in AXES]
        top, ws, l = weights(stats)
        st = jnp.where(lane < 64, top, l)
        for p in LINE:
            for v in range(n):
                j = p * n + v
                o = bc(ws[0], j) * acc[pl.ds(pl.multiple_of(a * 512 + (p * 128 + OFFS[c] + 8 * v), 8), 8), :]
                for r in AXES:
                    o = o + bc(ws[r + 1], j) * ra[c][r, p, 8 * v:8 * v + 8, :]
                redb[c][p, 8 * v:8 * v + 8, :] = o
            st_b[c, p] = st if p == 0 else pltpu.roll(st, 128 - p * n, 1)
        for r in FAR:
            for cp in copies_b(c, r):
                cp.start()

    for c in AXES:
        n = TILES[c]
        for r in NEAR:
            for cp in copies_b(c, r):
                cp.wait_recv()
        b = coord[(c + 1) % 3]
        me = coord[(c + 2) % 3]
        stats = [st_b[c, b]] + [rst_b[c, r] for r in AXES]
        top, ws, l = weights(stats)
        for v in range(n):
            o = bc(ws[0], v) * redb[c][b, 8 * v:8 * v + 8, :]
            for r in AXES:
                o = o + bc(ws[r + 1], v) * rb[c][r, 8 * v:8 * v + 8, :]
            rc[c][me, 8 * v:8 * v + 8, :] = o
        rst_c[c, me] = jnp.where(lane < 64, top, l)
        for r in FAR:
            for cp in copies_c(c, r, True):
                cp.start()

    for c in AXES:
        n = TILES[c]
        for r in NEAR:
            for cp in copies_c(c, r, False):
                cp.wait_recv()
        stats = [rst_c[c, i] for i in LINE]
        top, ws, l = weights(stats)
        base = (4 * coord[c] + coord[(c + 1) % 3]) * 128 + OFFS[c]
        for v in range(n):
            o = bc(ws[0], v) * rc[c][0, 8 * v:8 * v + 8, :]
            for i in range(1, 4):
                o = o + bc(ws[i], v) * rc[c][i, 8 * v:8 * v + 8, :]
            o = o / bc(l, 64 + v)
            attn[pl.ds(pl.multiple_of(base + 8 * v, 8), 8), :] = o.astype(BF16).astype(F32)
        for r in FAR:
            copy_gb(c, r, True).start()

    for c in AXES:
        for r in NEAR:
            copy_gb(c, r, False).wait_recv()
        for r in FAR:
            for cp in copies_ga(c, r, True):
                cp.start()
    for c in AXES:
        for r in NEAR:
            for cp in copies_ga(c, r, False):
                cp.wait_recv()
    for h in range(HEADS):
        lhs[:, h * 128:(h + 1) * 128] = attn[h * 64:(h + 1) * 64, :].astype(BF16)

    def t_copy(j):
        return pltpu.make_async_remote_copy(
            src_ref=pout.at[j], dst_ref=pin.at[j], send_sem=t_send.at[j], recv_sem=t_recv.at[j],
            device_id={"tp": 1 - tp}, device_id_type=MESH)

    def out_copy(j):
        cols = pl.ds(pl.multiple_of(j * CW, CW), CW)
        return pltpu.make_async_copy(hid.at[:, cols], out_h.at[:, cols], out_sem.at[j])

    def finish(j):
        cols = pl.ds(pl.multiple_of(j * CW, CW), CW)
        t_copy(j).wait_recv()
        hid[:, cols] = (hid[:, cols].astype(F32) + (pout[j] + pin[j])).astype(BF16)
        out_copy(j).start()

    def fin(j, carry):
        slot = (j + 5) % SLOTS
        wo_copy(j, slot).wait()
        pout[j] = jnp.dot(lhs[...], wbuf[slot], preferred_element_type=F32)
        t_copy(j).start()

        @pl.when(j + SLOTS < NCHUNK)
        def _():
            wo_copy(j + SLOTS, slot).start()

        @pl.when(j > 0)
        def _():
            finish(j - 1)
        return carry

    lax.fori_loop(0, NCHUNK, fin, 0)
    finish(NCHUNK - 1)

    for g in range(7):
        for r in NEAR:
            q_copy(g, r).wait_send()
    for c in AXES:
        for r in NEAR:
            for cp in copies_a(c, r) + copies_b(c, r) + copies_c(c, r, True) + copies_ga(c, r, True):
                cp.wait_send()
            copy_gb(c, r, True).wait_send()
    c_ko.wait()
    c_vo.wait()

    def drain(j, carry):
        t_copy(j).wait_send()
        out_copy(j).wait()
        return carry
    lax.fori_loop(0, NCHUNK, drain, 0)


def solution(mesh):
    cache_spec = P('dp', 'sp', 'tp', None)

    def local_step(hidden, lengths, k_cache, v_cache, norm_gain, w_query, w_key, w_value, w_out):
        shape = k_cache.shape
        kc = k_cache.reshape(BATCH * SEQ * KV, HEAD_DIM)
        vc = v_cache.reshape(BATCH * SEQ * KV, HEAD_DIM)
        any_ = pl.BlockSpec(memory_space=pl.ANY)
        dma = pltpu.SemaphoreType.DMA
        V = pltpu.VMEM
        n8 = [8 * n for n in TILES]
        rows, half, wide = HEADS * BATCH, D_MODEL // 2, (BATCH, D_MODEL)
        stat = V((3, 4, 8, HEAD_DIM), F32)

        def vec(*lead):
            return [V((*lead, n, HEAD_DIM), F32) for n in n8]

        scratch = [
            V(wide, BF16), V((1, D_MODEL), BF16), V(wide, BF16), V(kc.shape, BF16), V(vc.shape, BF16),
            V((rows + 2 * KV * BATCH, HEAD_DIM), F32), V((BATCH, HEAD_DIM), jnp.int32),
            V((rows, HEAD_DIM), F32), V((rows, HEAD_DIM), F32),
            stat, *vec(3, 4), stat, *vec(4), stat, *vec(3), stat, *vec(4), stat,
            V((rows, HEAD_DIM), F32), V((BATCH, half), BF16),
            V((NCHUNK, BATCH, CW), F32), V((NCHUNK, BATCH, CW), F32), V((SLOTS, half, CW), BF16),
            dma((NCHUNK,)), dma((SLOTS,)), dma((NCHUNK,)), dma((2,)),
        ]
        for shape_ in ((7, 3), (3, 3, 5), (3, 3, 2), (3, 3, 2), (3, 3), (3, 3, 4), (NCHUNK,)):
            scratch += [dma(shape_), dma(shape_)]
        out, ko, vo = pl.pallas_call(
            kernel,
            out_shape=(jax.ShapeDtypeStruct((BATCH, D_MODEL), BF16),
                       jax.ShapeDtypeStruct(kc.shape, BF16), jax.ShapeDtypeStruct(vc.shape, BF16)),
            in_specs=[pl.BlockSpec(memory_space=pltpu.SMEM)] + [any_] * 8,
            out_specs=(any_, any_, any_),
            scratch_shapes=scratch,
            compiler_params=pltpu.CompilerParams(
                collective_id=0, has_side_effects=True, vmem_limit_bytes=67043328),
        )(lengths, hidden, norm_gain.reshape(1, D_MODEL), kc, vc, w_query, w_key, w_value, w_out)
        return out, ko.reshape(shape), vo.reshape(shape)

    return jax.shard_map(
        local_step,
        mesh=mesh,
        in_specs=(P('dp', None), P('dp'), cache_spec, cache_spec, P(None), P(None, 'tp'), P(None, 'tp'), P(None, 'tp'), P('tp', None)),
        out_specs=(P('dp', None), cache_spec, cache_spec),
        check_vma=False,
    )
```

```python
import functools

import jax
import jax.numpy as jnp
from jax import lax
from jax.experimental import pallas as pl
from jax.experimental.pallas import tpu as pltpu
from jax.sharding import PartitionSpec as P

EPS = 1e-6
NEG_BIG = -1e30
MESH = pl.DeviceIdType.MESH
F32, BF16 = jnp.float32, jnp.bfloat16

BATCH, D_MODEL, HEAD_DIM = 64, 8192, 128
KV, HEADS, GROUP = 4, 32, 8
SEQ = 16
STRIDE = (1, 4, 16)
TILES = (5, 5, 6)
OFFS = (0, 40, 80)
SLOTS, NCHUNK, CW, LAG = 11, 16, 512, 3
GROUPS = ((24, 2, 2, 2), (0, 3, 2, 0), (12, 3, 2, 1), (2, 3, 1, 0), (14, 3, 1, 1), (32, 1, 1, 2), (36, 1, 1, 2))
AXES = (0, 1, 2)
LINE = (0, 1, 2, 3)
BLOCKS = 4
NEAR, FAR = (1, 3, 2), (2, 1, 3)


def kernel(lens, hid_h, gain_h, kc_h, vc_h, wq_h, wk_h, wv_h, wo_h,
           out_h, ko_h, vo_h,
           hid, gain, normed, kc, vc, qf, posm, acc, sfull,
           st_a, ra0, ra1, ra2, rst_a,
           b0_, b1_, b2_, st_b, rb0, rb1, rb2, rst_b,
           rc0, rc1, rc2, rst_c,
           attn, lhs, pout, pin, wbuf,
           in_sem, w_sem, out_sem, kv_sem,
           q_send, q_recv, a_send, a_recv, b_send, b_recv, c_send, c_recv,
           gb_send, gb_recv, ga_send, ga_recv, t_send, t_recv):
    sp = lax.axis_index("sp")
    tp = lax.axis_index("tp")
    coord = [sp % 4, (sp // 4) % 4, sp // 16]
    ra, redb, rb, rc = (ra0, ra1, ra2), (b0_, b1_, b2_), (rb0, rb1, rb2), (rc0, rc1, rc2)

    def peer(axis, r):
        c = coord[axis]
        t = (c + r) % 4
        return sp + (t - c) * STRIDE[axis], t

    c_hid = pltpu.make_async_copy(hid_h, hid, in_sem.at[0])
    c_gain = pltpu.make_async_copy(gain_h, gain, in_sem.at[1])
    c_hid.start()
    c_gain.start()
    x, y, z = coord

    def wcol(slot, half, hbm, col, width, at, sem):
        return pltpu.make_async_copy(
            hbm.at[pl.ds(half * 4096, 4096), pl.ds(pl.multiple_of(col, 128), width)],
            wbuf.at[slot, :, pl.ds(half * 256 + at, width)], sem)

    wq_copies = []
    chunks = (
        ((wq_h, (24 + 2 * z) * 128, 256, 0),),
        ((wq_h, (3 * x) * 128, 256, 0),),
        ((wq_h, (12 + 3 * y) * 128, 256, 0),),
        ((wq_h, (3 * x + 2) * 128, 128, 0), (wq_h, (12 + 3 * y + 2) * 128, 128, 128)),
        ((wk_h, z * 128, 128, 0), (wv_h, z * 128, 128, 128)),
    )
    nsem = 2
    for s, parts in enumerate(chunks):
        cs = []
        for half in range(2):
            for (hbm, col, width, at) in parts:
                cs.append(wcol(s, half, hbm, col, width, at, in_sem.at[nsem]))
                nsem += 1
        for c in cs:
            c.start()
        wq_copies.append(cs)
    c_k = pltpu.make_async_copy(kc_h, kc, kv_sem.at[0])
    c_v = pltpu.make_async_copy(vc_h, vc, kv_sem.at[1])
    c_k.start()
    c_v.start()

    barrier = pltpu.get_barrier_semaphore()
    for axis in AXES:
        for r in NEAR:
            pl.semaphore_signal(barrier, inc=1, device_id={"sp": peer(axis, r)[0]}, device_id_type=MESH)
    pl.semaphore_signal(barrier, inc=1, device_id={"tp": 1 - tp}, device_id_type=MESH)

    c_hid.wait()
    c_gain.wait()
    ss = jnp.zeros((BATCH, 128), F32)
    for c in range(0, D_MODEL, 512):
        h = hid[:, c:c + 512].astype(F32)
        h = h * h
        ss = ss + ((h[:, 0:128] + h[:, 128:256]) + (h[:, 256:384] + h[:, 384:512]))
    gf = gain[...].astype(F32)
    inv = lax.rsqrt(jnp.sum(ss, axis=1, keepdims=True) * (1.0 / D_MODEL) + EPS)
    for c in range(0, D_MODEL, 512):
        h = hid[:, c:c + 512].astype(F32)
        g = jnp.concatenate([gf[k:k + 1] for k in range(c // HEAD_DIM, (c + 512) // HEAD_DIM)], axis=1)
        normed[:, c:c + 512] = (h * inv * g).astype(BF16)

    def q_copy(g, r, own=True):
        base, mult, count, axis = GROUPS[g]
        c = coord[axis] if own else (coord[axis] + 4 - r) % 4
        rows = pl.ds(pl.multiple_of((base + mult * c) * BATCH, BATCH), count * BATCH)
        return pltpu.make_async_remote_copy(
            src_ref=qf.at[rows], dst_ref=qf.at[rows],
            send_sem=q_send.at[g, r - 1], recv_sem=q_recv.at[g, r - 1],
            device_id={"sp": peer(axis, r)[0]}, device_id_type=MESH)

    def wo_copy(j, slot):
        return pltpu.make_async_copy(
            wo_h.at[:, pl.ds(pl.multiple_of(j * CW, CW), CW)], wbuf.at[slot], w_sem.at[slot])

    def put(g, k, val):
        base, mult, count, axis = GROUPS[g]
        rows = pl.ds(pl.multiple_of((base + mult * coord[axis] + k) * BATCH, BATCH), BATCH)
        qf[rows, :] = val.astype(BF16).astype(F32)

    plan = (((0, 0), (0, 1)), ((1, 0), (1, 1)), ((2, 0), (2, 1)), ((3, 0), (4, 0)), ((5, 0), (6, 0)))
    for s in range(5):
        for c in wq_copies[s]:
            c.wait()
        if s == 4:
            for j in range(6):
                wo_copy(j, 5 + j).start()
        res = (jnp.dot(normed[:, 0:4096], wbuf[s, :, 0:256], preferred_element_type=F32)
               + jnp.dot(normed[:, 4096:8192], wbuf[s, :, 256:512], preferred_element_type=F32))
        (g0, k0), (g1, k1) = plan[s]
        put(g0, k0, res[:, 0:128])
        put(g1, k1, res[:, 128:256])
        if s == 0:
            pl.semaphore_wait(barrier, 10)
        for g in sorted({g0, g1}):
            for r in FAR:
                q_copy(g, r).start()
    for j in range(6, 11):
        wo_copy(j, j - 6).start()

    row = lax.broadcasted_iota(jnp.int32, (64, 128), 0)
    col = lax.broadcasted_iota(jnp.int32, (64, 128), 1)
    own = (row // 32 == col // 64) & ((row % 32) // GROUP == col % KV)
    posm[...] = jnp.where(own, sp * SEQ + (col % 64) // KV, 1 << 30)

    c_k.wait()
    c_v.wait()
    for g in range(7):
        for r in NEAR:
            q_copy(g, r, False).wait_recv()

    scale = HEAD_DIM ** -0.5
    rpos = sp * SEQ + lax.broadcasted_iota(jnp.int32, (64, 128), 0) // KV
    lane = lax.broadcasted_iota(jnp.int32, (8, 128), 1)
    UN = 4

    def attn_body(i, carry):
        lens_, qs, ks, vs = [], [], [], []
        for u in range(UN):
            b = (i * UN + u) * 2
            l0, l1 = lens[b], lens[b + 1]
            lens_.append((l0, l1))
            q = jnp.concatenate([qf[pl.ds(b, 32, stride=64), :], qf[pl.ds(b + 1, 32, stride=64), :]], axis=0)
            qs.append(q.astype(BF16))
            for ref, base, dst in ((kc, 32, ks), (vc, 36, vs)):
                both = []
                for e, ln in ((0, l0), (1, l1)):
                    new = qf[pl.ds(base * 64 + b + e, 4, stride=64), :]
                    new8 = jnp.concatenate([new, new], axis=0)
                    new64 = jnp.concatenate([new8] * 8, axis=0)
                    old = ref[pl.ds(pl.multiple_of((b + e) * 64, 64), 64), :]
                    both.append(jnp.where(rpos == ln, new64, old.astype(F32)).astype(BF16))
                val = jnp.concatenate(both, axis=0)
                ref[pl.ds(pl.multiple_of(b * 64, 128), 128), :] = val
                dst.append(val)
        ss_ = [lax.dot_general(qs[u], ks[u], (((1,), (1,)), ((), ())), preferred_element_type=F32) for u in range(UN)]
        ps, sts = [], []
        for u in range(UN):
            l0, l1 = lens_[u]
            pm = posm[...]
            valid = jnp.concatenate([pm[0:32] <= l0, pm[32:64] <= l1], axis=0)
            s = jnp.where(valid, ss_[u] * scale, NEG_BIG)
            m = jnp.max(s, axis=1, keepdims=True)
            e = jnp.where(valid, jnp.exp(s - m), 0.0)
            l = jnp.sum(e, axis=1, keepdims=True)
            ps.append(e.astype(BF16))
            col2 = lax.broadcasted_iota(jnp.int32, (64, 128), 1)
            sts.append(jnp.where(col2 < 64, m, l))
        for u in range(UN):
            b = (i * UN + u) * 2
            o = jnp.dot(ps[u], vs[u], preferred_element_type=F32)
            acc[pl.ds(b, 32, stride=64), :] = o[0:32]
            acc[pl.ds(b + 1, 32, stride=64), :] = o[32:64]
            sfull[pl.ds(b, 32, stride=64), :] = sts[u][0:32]
            sfull[pl.ds(b + 1, 32, stride=64), :] = sts[u][32:64]
        return carry

    lax.fori_loop(0, BATCH // 2 // UN, attn_body, 0)

    c_ko = pltpu.make_async_copy(kc, ko_h, kv_sem.at[0])
    c_vo = pltpu.make_async_copy(vc, vo_h, kv_sem.at[1])
    c_ko.start()
    c_vo.start()

    lane64 = lane % 64
    for c in AXES:
        n = TILES[c]
        for a in LINE:
            st = jnp.zeros((8, 128), F32)
            for p in LINE:
                for v in range(n):
                    r0 = (4 * a + p) * 128 + OFFS[c] + 8 * v
                    st = jnp.where(lane64 == p * n + v, sfull[r0:r0 + 8, :], st)
            st_a[c, a] = st

    def remote(src, dst, ss_sem, rs_sem, dev):
        return pltpu.make_async_remote_copy(
            src_ref=src, dst_ref=dst, send_sem=ss_sem, recv_sem=rs_sem,
            device_id={"sp": dev}, device_id_type=MESH)

    def copies_a(c, r):
        n = TILES[c]
        dev, t = peer(c, r)
        out = [remote(st_a.at[c, t], rst_a.at[c, r - 1], a_send.at[c, r - 1, 4], a_recv.at[c, r - 1, 4], dev)]
        for p in LINE:
            src = acc.at[pl.ds(pl.multiple_of(t * 512 + (p * 128 + OFFS[c]), 8), 8 * n)]
            out.append(remote(src, ra[c].at[r - 1, p], a_send.at[c, r - 1, p], a_recv.at[c, r - 1, p], dev))
        return out

    def copies_b(c, r):
        dev, t = peer((c + 1) % 3, r)
        return [remote(redb[c].at[t], rb[c].at[r - 1], b_send.at[c, r - 1, 0], b_recv.at[c, r - 1, 0], dev),
                remote(st_b.at[c, t], rst_b.at[c, r - 1], b_send.at[c, r - 1, 1], b_recv.at[c, r - 1, 1], dev)]

    def copies_c(c, r, own):
        axis = (c + 2) % 3
        dev, t = peer(axis, r)
        at = coord[axis] if own else (coord[axis] + 4 - r) % 4
        return [remote(rc[c].at[at], rc[c].at[at], c_send.at[c, r - 1, 0], c_recv.at[c, r - 1, 0], dev),
                remote(rst_c.at[c, at], rst_c.at[c, at], c_send.at[c, r - 1, 1], c_recv.at[c, r - 1, 1], dev)]

    def copy_gb(c, r, own):
        axis = (c + 1) % 3
        dev, t = peer(axis, r)
        at = coord[axis] if own else (coord[axis] + 4 - r) % 4
        rows = pl.ds(pl.multiple_of((4 * coord[c] + at) * 128 + OFFS[c], 8), 8 * TILES[c])
        return remote(attn.at[rows], attn.at[rows], gb_send.at[c, r - 1], gb_recv.at[c, r - 1], dev)

    def copies_ga(c, r, own):
        dev, t = peer(c, r)
        at = coord[c] if own else (coord[c] + 4 - r) % 4
        out = []
        for p in LINE:
            rows = pl.ds(pl.multiple_of((4 * at + p) * 128 + OFFS[c], 8), 8 * TILES[c])
            out.append(remote(attn.at[rows], attn.at[rows], ga_send.at[c, r - 1, p], ga_recv.at[c, r - 1, p], dev))
        return out

    for r in FAR:
        for c in AXES:
            for cp in copies_a(c, r):
                cp.start()

    def weights(stats):
        top = functools.reduce(jnp.maximum, stats)
        ws = [jnp.exp(s - top) for s in stats]
        l = sum(pltpu.roll(w, 64, 1) * s for w, s in zip(ws, stats))
        return top, ws, l

    def bc(w, j):
        return jnp.broadcast_to(w[:, j:j + 1], (8, 128))

    for c in AXES:
        n = TILES[c]
        for r in NEAR:
            for cp in copies_a(c, r):
                cp.wait_recv()
        a = coord[c]
        stats = [st_a[c, a]] + [rst_a[c, r] for r in AXES]
        top, ws, l = weights(stats)
        st = jnp.where(lane < 64, top, l)
        for p in LINE:
            for v in range(n):
                j = p * n + v
                o = bc(ws[0], j) * acc[pl.ds(pl.multiple_of(a * 512 + (p * 128 + OFFS[c] + 8 * v), 8), 8), :]
                for r in AXES:
                    o = o + bc(ws[r + 1], j) * ra[c][r, p, 8 * v:8 * v + 8, :]
                redb[c][p, 8 * v:8 * v + 8, :] = o
            st_b[c, p] = st if p == 0 else pltpu.roll(st, 128 - p * n, 1)
        for r in FAR:
            for cp in copies_b(c, r):
                cp.start()

    for c in AXES:
        n = TILES[c]
        for r in NEAR:
            for cp in copies_b(c, r):
                cp.wait_recv()
        b = coord[(c + 1) % 3]
        me = coord[(c + 2) % 3]
        stats = [st_b[c, b]] + [rst_b[c, r] for r in AXES]
        top, ws, l = weights(stats)
        for v in range(n):
            o = bc(ws[0], v) * redb[c][b, 8 * v:8 * v + 8, :]
            for r in AXES:
                o = o + bc(ws[r + 1], v) * rb[c][r, 8 * v:8 * v + 8, :]
            rc[c][me, 8 * v:8 * v + 8, :] = o
        rst_c[c, me] = jnp.where(lane < 64, top, l)
        for r in FAR:
            for cp in copies_c(c, r, True):
                cp.start()

    for c in AXES:
        n = TILES[c]
        for r in NEAR:
            for cp in copies_c(c, r, False):
                cp.wait_recv()
        stats = [rst_c[c, i] for i in LINE]
        top, ws, l = weights(stats)
        base = (4 * coord[c] + coord[(c + 1) % 3]) * 128 + OFFS[c]
        for v in range(n):
            o = bc(ws[0], v) * rc[c][0, 8 * v:8 * v + 8, :]
            for i in range(1, 4):
                o = o + bc(ws[i], v) * rc[c][i, 8 * v:8 * v + 8, :]
            o = o / bc(l, 64 + v)
            attn[pl.ds(pl.multiple_of(base + 8 * v, 8), 8), :] = o.astype(BF16).astype(F32)
        for r in FAR:
            copy_gb(c, r, True).start()

    for c in AXES:
        for r in NEAR:
            copy_gb(c, r, False).wait_recv()
        for r in FAR:
            for cp in copies_ga(c, r, True):
                cp.start()
    for c in AXES:
        for r in NEAR:
            for cp in copies_ga(c, r, False):
                cp.wait_recv()
    for h in range(HEADS):
        lhs[:, h * 128:(h + 1) * 128] = attn[h * 64:(h + 1) * 64, :].astype(BF16)

    def t_copy(j):
        return pltpu.make_async_remote_copy(
            src_ref=pout.at[j], dst_ref=pin.at[j], send_sem=t_send.at[j], recv_sem=t_recv.at[j],
            device_id={"tp": 1 - tp}, device_id_type=MESH)

    def out_copy(j):
        cols = pl.ds(pl.multiple_of(j * CW, CW), CW)
        return pltpu.make_async_copy(hid.at[:, cols], out_h.at[:, cols], out_sem.at[j])

    def finish(j):
        cols = pl.ds(pl.multiple_of(j * CW, CW), CW)
        t_copy(j).wait_recv()
        hid[:, cols] = (hid[:, cols].astype(F32) + (pout[j] + pin[j])).astype(BF16)
        out_copy(j).start()

    def fin(j, carry):
        slot = (j + 5) % SLOTS
        wo_copy(j, slot).wait()
        pout[j] = jnp.dot(lhs[...], wbuf[slot], preferred_element_type=F32)
        t_copy(j).start()

        @pl.when(j + SLOTS < NCHUNK)
        def _():
            wo_copy(j + SLOTS, slot).start()

        @pl.when(j >= LAG)
        def _():
            finish(j - LAG)
        return carry

    lax.fori_loop(0, NCHUNK, fin, 0)
    for j in range(NCHUNK - LAG, NCHUNK):
        finish(j)

    for g in range(7):
        for r in NEAR:
            q_copy(g, r).wait_send()
    for c in AXES:
        for r in NEAR:
            for cp in copies_a(c, r) + copies_b(c, r) + copies_c(c, r, True) + copies_ga(c, r, True):
                cp.wait_send()
            copy_gb(c, r, True).wait_send()
    c_ko.wait()
    c_vo.wait()

    def drain(j, carry):
        t_copy(j).wait_send()
        out_copy(j).wait()
        return carry
    lax.fori_loop(0, NCHUNK, drain, 0)


def copy_out(*refs):
    n = (len(refs) - 2) // 3
    ins, outs, bufs, i_sem, o_sem = refs[:n], refs[n:2 * n], refs[2 * n:3 * n], refs[-2], refs[-1]
    moves = []
    for k in range(n):
        step = ins[k].shape[0] // BLOCKS
        for j in range(BLOCKS):
            rows = pl.ds(j * step, step)
            moves.append((pltpu.make_async_copy(ins[k].at[rows], bufs[k].at[rows], i_sem.at[k, j]),
                          pltpu.make_async_copy(bufs[k].at[rows], outs[k].at[rows], o_sem.at[k, j])))
    for a, _ in moves:
        a.start()
    for a, b in moves:
        a.wait()
        b.start()
    for _, b in moves:
        b.wait()


def solution(mesh):
    cache_spec = P('dp', 'sp', 'tp', None)

    def local_step(hidden, lengths, k_cache, v_cache, norm_gain, w_query, w_key, w_value, w_out):
        shape = k_cache.shape
        kc = k_cache.reshape(BATCH * SEQ * KV, HEAD_DIM)
        vc = v_cache.reshape(BATCH * SEQ * KV, HEAD_DIM)
        any_ = pl.BlockSpec(memory_space=pl.ANY)
        dma = pltpu.SemaphoreType.DMA
        V = pltpu.VMEM
        n8 = [8 * n for n in TILES]
        rows, half, wide = HEADS * BATCH, D_MODEL // 2, (BATCH, D_MODEL)
        stat = V((3, 4, 8, HEAD_DIM), F32)

        def vec(*lead):
            return [V((*lead, n, HEAD_DIM), F32) for n in n8]

        scratch = [
            V(wide, BF16), V((D_MODEL // HEAD_DIM, HEAD_DIM), BF16), V(wide, BF16), V(kc.shape, BF16), V(vc.shape, BF16),
            V((rows + 2 * KV * BATCH, HEAD_DIM), F32), V((BATCH, HEAD_DIM), jnp.int32),
            V((rows, HEAD_DIM), F32), V((rows, HEAD_DIM), F32),
            stat, *vec(3, 4), stat, *vec(4), stat, *vec(3), stat, *vec(4), stat,
            V((rows, HEAD_DIM), F32), V((BATCH, half), BF16),
            V((NCHUNK, BATCH, CW), F32), V((NCHUNK, BATCH, CW), F32), V((SLOTS, half, CW), BF16),
            dma((NCHUNK,)), dma((SLOTS,)), dma((NCHUNK,)), dma((2,)),
        ]
        for shape_ in ((7, 3), (3, 3, 5), (3, 3, 2), (3, 3, 2), (3, 3), (3, 3, 4), (NCHUNK,)):
            scratch += [dma(shape_), dma(shape_)]
        res = pl.pallas_call(
            kernel,
            out_shape=(jax.ShapeDtypeStruct((BATCH, D_MODEL), BF16),
                       jax.ShapeDtypeStruct(kc.shape, BF16), jax.ShapeDtypeStruct(vc.shape, BF16)),
            in_specs=[pl.BlockSpec(memory_space=pltpu.SMEM)] + [any_] * 8,
            out_specs=(any_, any_, any_),
            scratch_shapes=scratch,
            compiler_params=pltpu.CompilerParams(
                collective_id=0, has_side_effects=True, vmem_limit_bytes=67043328),
        )(lengths, hidden, norm_gain.reshape(D_MODEL // HEAD_DIM, HEAD_DIM), kc, vc, w_query, w_key, w_value, w_out)
        out, ko, vo = pl.pallas_call(
            copy_out,
            out_shape=tuple(jax.ShapeDtypeStruct(r.shape, r.dtype) for r in res),
            in_specs=[any_] * len(res),
            out_specs=(any_,) * len(res),
            scratch_shapes=[V(r.shape, r.dtype) for r in res] + [dma((len(res), BLOCKS))] * 2,
        )(*res)
        return out, ko.reshape(shape), vo.reshape(shape)

    return jax.shard_map(
        local_step,
        mesh=mesh,
        in_specs=(P('dp', None), P('dp'), cache_spec, cache_spec, P(None), P(None, 'tp'), P(None, 'tp'), P(None, 'tp'), P('tp', None)),
        out_specs=(P('dp', None), cache_spec, cache_spec),
        check_vma=False,
    )
```

```python
import functools

import jax
import jax.numpy as jnp
from jax import lax
from jax.experimental import pallas as pl
from jax.experimental.pallas import tpu as pltpu
from jax.sharding import PartitionSpec as P

EPS = 1e-6
NEG_BIG = -1e30
MESH = pl.DeviceIdType.MESH
F32, BF16 = jnp.float32, jnp.bfloat16

BATCH, D_MODEL, HEAD_DIM = 64, 8192, 128
KV, HEADS, GROUP = 4, 32, 8
SEQ = 16
STRIDE = (1, 4, 16)
FIRST = (0, 12, 24)
NH = (3, 3, 2)
TILES = (6, 6, 4)
SLOTS, CUTS, NCHUNK, CW = 11, 4, 16, 512
WIDE = NCHUNK * CW // CUTS
ORDER = (0, 1, 3, 2)
BGROUP = 16
GROUPS = ((24, 2, 2, 2), (0, 3, 2, 0), (12, 3, 2, 1), (2, 3, 1, 0), (14, 3, 1, 1), (32, 1, 1, 2), (36, 1, 1, 2))
AXES = (0, 1, 2)
LINE = (0, 1, 2, 3)
BLOCKS = 4
NEAR, FAR = (1, 3, 2), (2, 1, 3)


def kernel(lens, hid_h, gain_h, kc_h, vc_h, wq_h, wk_h, wv_h, wo_h,
           out_h, ko_h, vo_h,
           hid, gain, normed, kc, vc, qf, posm, acc, sfull,
           st_a, ra0, ra1, ra2, rst_a,
           b0_, b1_, b2_, st_b, rb0, rb1, rb2, rst_b,
           rc0, rc1, rc2, rst_c,
           attn, lhs, pout, pin, wbuf,
           in_sem, w_sem, out_sem, kv_sem,
           q_send, q_recv, a_send, a_recv, b_send, b_recv, c_send, c_recv,
           gb_send, gb_recv, ga_send, ga_recv, t_send, t_recv):
    sp = lax.axis_index("sp")
    tp = lax.axis_index("tp")
    coord = [sp % 4, (sp // 4) % 4, sp // 16]
    ra, redb, rb, rc = (ra0, ra1, ra2), (b0_, b1_, b2_), (rb0, rb1, rb2), (rc0, rc1, rc2)

    def peer(axis, r):
        c = coord[axis]
        t = (c + r) % 4
        return sp + (t - c) * STRIDE[axis], t

    c_hid = pltpu.make_async_copy(hid_h, hid, in_sem.at[0])
    c_gain = pltpu.make_async_copy(gain_h, gain, in_sem.at[1])
    c_hid.start()
    c_gain.start()
    x, y, z = coord

    KB = 1024

    def wcols(slot, hbm, col, width, at, base):
        return [pltpu.make_async_copy(
            hbm.at[pl.ds(k * KB, KB), pl.ds(pl.multiple_of(col, HEAD_DIM), width)],
            wbuf.at[slot, :, pl.ds(k * 256 + at, width)], in_sem.at[base + k]) for k in range(D_MODEL // KB)]

    wq_copies = []
    chunks = (
        ((wq_h, 24 + 2 * z),),
        ((wk_h, z), (wv_h, z)),
        ((wq_h, 3 * x),),
        ((wq_h, 12 + 3 * y),),
        ((wq_h, 3 * x + 2), (wq_h, 12 + 3 * y + 2)),
    )
    nsem = 2
    for i, parts in enumerate(chunks):
        cs = []
        width = 256 // len(parts)
        for k, (hbm, head) in enumerate(parts):
            cs += wcols(i, hbm, head * HEAD_DIM, width, k * width, nsem)
            nsem += D_MODEL // KB
        for c in cs:
            c.start()
        wq_copies.append(cs)
    c_k = pltpu.make_async_copy(kc_h, kc, kv_sem.at[0])
    c_v = pltpu.make_async_copy(vc_h, vc, kv_sem.at[1])

    barrier = pltpu.get_barrier_semaphore()
    for axis in AXES:
        for r in NEAR:
            pl.semaphore_signal(barrier, inc=1, device_id={"sp": peer(axis, r)[0]}, device_id_type=MESH)
    pl.semaphore_signal(barrier, inc=1, device_id={"tp": 1 - tp}, device_id_type=MESH)

    c_hid.wait()
    c_gain.wait()
    ss = jnp.zeros((BATCH, 128), F32)
    for c in range(0, D_MODEL, 512):
        h = hid[:, c:c + 512].astype(F32)
        h = h * h
        ss = ss + ((h[:, 0:128] + h[:, 128:256]) + (h[:, 256:384] + h[:, 384:512]))
    gf = gain[...].astype(F32)
    inv = lax.rsqrt(jnp.sum(ss, axis=1, keepdims=True) * (1.0 / D_MODEL) + EPS)
    for c in range(0, D_MODEL, 512):
        h = hid[:, c:c + 512].astype(F32)
        g = jnp.concatenate([gf[k:k + 1] for k in range(c // HEAD_DIM, (c + 512) // HEAD_DIM)], axis=1)
        normed[:, c:c + 512] = (h * inv * g).astype(BF16)

    def q_copy(g, r, own=True):
        base, mult, count, axis = GROUPS[g]
        c = coord[axis] if own else (coord[axis] + 4 - r) % 4
        rows = pl.ds(pl.multiple_of((base + mult * c) * BATCH, BATCH), count * BATCH)
        return pltpu.make_async_remote_copy(
            src_ref=qf.at[rows], dst_ref=qf.at[rows],
            send_sem=q_send.at[g, r - 1], recv_sem=q_recv.at[g, r - 1],
            device_id={"sp": peer(axis, r)[0]}, device_id_type=MESH)

    def head0(c, r):
        return FIRST[c] + NH[c] * ((coord[c] + 4 - r) % 4)

    def wo_copies(i):
        slot, r, at, out = (i + 5) % SLOTS, ORDER[i // CUTS], 0, []
        for c in AXES:
            n = NH[c] * HEAD_DIM
            rows = pl.ds(pl.multiple_of(head0(c, r) * HEAD_DIM, HEAD_DIM), n)
            out.append(pltpu.make_async_copy(
                wo_h.at[rows, pl.ds((i % CUTS) * WIDE, WIDE)], wbuf.at[slot, pl.ds(at, n), :], w_sem.at[slot, c]))
            at += n
        return out

    def put(g, k, val):
        base, mult, count, axis = GROUPS[g]
        rows = pl.ds(pl.multiple_of((base + mult * coord[axis] + k) * BATCH, BATCH), BATCH)
        qf[rows, :] = val.astype(BF16).astype(F32)

    plan = (((0, 0), (0, 1)), ((5, 0), (6, 0)), ((1, 0), (1, 1)), ((2, 0), (2, 1)), ((3, 0), (4, 0)))
    for i in range(5):
        for c in wq_copies[i]:
            c.wait()
        if i == 2:
            c_k.start()
            c_v.start()
        if i == 4:
            for j in range(6):
                for c in wo_copies(j):
                    c.start()
        res = sum(jnp.dot(normed[:, k * KB:(k + 1) * KB], wbuf[i, :, k * 256:(k + 1) * 256], preferred_element_type=F32)
                  for k in range(D_MODEL // KB))
        (g0, k0), (g1, k1) = plan[i]
        put(g0, k0, res[:, :HEAD_DIM])
        put(g1, k1, res[:, HEAD_DIM:])
        if i == 0:
            pl.semaphore_wait(barrier, 10)
        for g in sorted({g0, g1}):
            for r in FAR:
                q_copy(g, r).start()
    for j in range(6, SLOTS):
        for c in wo_copies(j):
            c.start()

    row = lax.broadcasted_iota(jnp.int32, (64, 128), 0)
    col = lax.broadcasted_iota(jnp.int32, (64, 128), 1)
    own = (row // 32 == col // 64) & ((row % 32) // GROUP == col % KV)
    posm[...] = jnp.where(own, sp * SEQ + (col % 64) // KV, 1 << 30)

    c_k.wait()
    c_v.wait()
    for g in range(7):
        for r in NEAR:
            q_copy(g, r, False).wait_recv()

    scale = HEAD_DIM ** -0.5
    rpos = sp * SEQ + lax.broadcasted_iota(jnp.int32, (64, 128), 0) // KV
    lane = lax.broadcasted_iota(jnp.int32, (8, 128), 1)
    UN = 4
    acc3 = acc.reshape(HEADS, BATCH, HEAD_DIM)

    def remote(src, dst, ss_sem, rs_sem, dev):
        return pltpu.make_async_remote_copy(
            src_ref=src, dst_ref=dst, send_sem=ss_sem, recv_sem=rs_sem,
            device_id={"sp": dev}, device_id_type=MESH)

    def copy_a(c, r, g):
        dev, t = peer(c, r)
        seqs = pl.ds(pl.multiple_of(g * BGROUP, BGROUP), BGROUP)
        return remote(acc3.at[pl.ds(FIRST[c] + NH[c] * t, NH[c]), seqs], ra[c].at[r - 1, :, seqs],
                      a_send.at[c, r - 1, g], a_recv.at[c, r - 1, g], dev)

    def copy_sa(c, r):
        dev, t = peer(c, r)
        return remote(st_a.at[c, t], rst_a.at[c, r - 1], a_send.at[c, r - 1, 4], a_recv.at[c, r - 1, 4], dev)

    def attn_part(i):
        lens_, qs, ks, vs = [], [], [], []
        for u in range(UN):
            b = (i * UN + u) * 2
            l0, l1 = lens[b], lens[b + 1]
            lens_.append((l0, l1))
            q = jnp.concatenate([qf[pl.ds(b, 32, stride=64), :], qf[pl.ds(b + 1, 32, stride=64), :]], axis=0)
            qs.append(q.astype(BF16))
            for ref, base, dst in ((kc, 32, ks), (vc, 36, vs)):
                both = []
                for e, ln in ((0, l0), (1, l1)):
                    new = qf[pl.ds(base * 64 + b + e, 4, stride=64), :]
                    new8 = jnp.concatenate([new, new], axis=0)
                    new64 = jnp.concatenate([new8] * 8, axis=0)
                    old = ref[pl.ds(pl.multiple_of((b + e) * 64, 64), 64), :]
                    both.append(jnp.where(rpos == ln, new64, old.astype(F32)).astype(BF16))
                val = jnp.concatenate(both, axis=0)
                ref[pl.ds(pl.multiple_of(b * 64, 128), 128), :] = val
                dst.append(val)
        ss_ = [lax.dot_general(qs[u], ks[u], (((1,), (1,)), ((), ())), preferred_element_type=F32) for u in range(UN)]
        ps, sts = [], []
        for u in range(UN):
            l0, l1 = lens_[u]
            pm = posm[...]
            valid = jnp.concatenate([pm[0:32] <= l0, pm[32:64] <= l1], axis=0)
            s = jnp.where(valid, ss_[u] * scale, NEG_BIG)
            m = jnp.max(s, axis=1, keepdims=True)
            e = jnp.where(valid, jnp.exp(s - m), 0.0)
            l = jnp.sum(e, axis=1, keepdims=True)
            ps.append(e.astype(BF16))
            col2 = lax.broadcasted_iota(jnp.int32, (64, 128), 1)
            sts.append(jnp.where(col2 < 64, m, l))
        for u in range(UN):
            b = (i * UN + u) * 2
            o = jnp.dot(ps[u], vs[u], preferred_element_type=F32)
            acc[pl.ds(b, 32, stride=64), :] = o[0:32]
            acc[pl.ds(b + 1, 32, stride=64), :] = o[32:64]
            sfull[pl.ds(b, 32, stride=64), :] = sts[u][0:32]
            sfull[pl.ds(b + 1, 32, stride=64), :] = sts[u][32:64]

    def attn_body(g, carry):
        per = BGROUP // 2 // UN
        for k in range(per):
            attn_part(g * per + k)
        for r in FAR:
            for c in AXES:
                copy_a(c, r, g).start()
        return carry

    lax.fori_loop(0, BATCH // BGROUP, attn_body, 0)

    c_ko = pltpu.make_async_copy(kc, ko_h, kv_sem.at[0])
    c_vo = pltpu.make_async_copy(vc, vo_h, kv_sem.at[1])
    c_ko.start()
    c_vo.start()

    lane64 = lane % 64
    for c in AXES:
        for a in LINE:
            st = jnp.zeros((8, 128), F32)
            for j in range(8 * NH[c]):
                r0 = (FIRST[c] + NH[c] * a) * BATCH + 8 * j
                st = jnp.where(lane64 == j, sfull[r0:r0 + 8, :], st)
            st_a[c, a] = st

    def copies_b(c, r):
        dev, t = peer((c + 1) % 3, r)
        return [remote(redb[c].at[t], rb[c].at[r - 1], b_send.at[c, r - 1, 0], b_recv.at[c, r - 1, 0], dev),
                remote(st_b.at[c, t], rst_b.at[c, r - 1], b_send.at[c, r - 1, 1], b_recv.at[c, r - 1, 1], dev)]

    def copies_c(c, r, own):
        axis = (c + 2) % 3
        dev, t = peer(axis, r)
        at = coord[axis] if own else (coord[axis] + 4 - r) % 4
        return [remote(rc[c].at[at], rc[c].at[at], c_send.at[c, r - 1, 0], c_recv.at[c, r - 1, 0], dev),
                remote(rst_c.at[c, at], rst_c.at[c, at], c_send.at[c, r - 1, 1], c_recv.at[c, r - 1, 1], dev)]

    def piece(c, ra_, rb_):
        b = (coord[(c + 1) % 3] + 4 - rb_) % 4
        return pl.ds(pl.multiple_of(head0(c, ra_) * BATCH + b * (8 * TILES[c]), 8), 8 * TILES[c])

    def copy_gb(c, r, own):
        rows = piece(c, 0, 0 if own else r)
        return remote(attn.at[rows], attn.at[rows], gb_send.at[c, r - 1], gb_recv.at[c, r - 1], peer((c + 1) % 3, r)[0])

    def copy_ga(c, r, q, own):
        rows = piece(c, 0 if own else r, q)
        return remote(attn.at[rows], attn.at[rows], ga_send.at[c, r - 1, q], ga_recv.at[c, r - 1, q], peer(c, r)[0])

    for r in FAR:
        for c in AXES:
            copy_sa(c, r).start()

    def weights(stats):
        top = functools.reduce(jnp.maximum, stats)
        ws = [jnp.exp(s - top) for s in stats]
        l = sum(pltpu.roll(w, 64, 1) * s for w, s in zip(ws, stats))
        return top, ws, l

    def bc(w, j):
        return jnp.broadcast_to(w[:, j:j + 1], (8, 128))

    for c in AXES:
        n = TILES[c]
        for r in NEAR:
            for g in range(BATCH // BGROUP):
                copy_a(c, r, g).wait_recv()
            copy_sa(c, r).wait_recv()
        a = coord[c]
        stats = [st_a[c, a]] + [rst_a[c, r] for r in AXES]
        top, ws, l = weights(stats)
        st = jnp.where(lane < 64, top, l)
        for j in range(8 * NH[c]):
            p, v, h, k = j // n, j % n, j // 8, j % 8
            o = bc(ws[0], j) * acc[pl.ds(pl.multiple_of(head0(c, 0) * BATCH + 8 * j, 8), 8), :]
            for r in AXES:
                o = o + bc(ws[r + 1], j) * ra[c][r, h, 8 * k:8 * k + 8, :]
            redb[c][p, 8 * v:8 * v + 8, :] = o
        for p in LINE:
            st_b[c, p] = st if p == 0 else pltpu.roll(st, 128 - p * n, 1)
        for r in FAR:
            for cp in copies_b(c, r):
                cp.start()

    for c in AXES:
        n = TILES[c]
        for r in NEAR:
            for cp in copies_b(c, r):
                cp.wait_recv()
        b = coord[(c + 1) % 3]
        me = coord[(c + 2) % 3]
        stats = [st_b[c, b]] + [rst_b[c, r] for r in AXES]
        top, ws, l = weights(stats)
        for v in range(n):
            o = bc(ws[0], v) * redb[c][b, 8 * v:8 * v + 8, :]
            for r in AXES:
                o = o + bc(ws[r + 1], v) * rb[c][r, 8 * v:8 * v + 8, :]
            rc[c][me, 8 * v:8 * v + 8, :] = o
        rst_c[c, me] = jnp.where(lane < 64, top, l)
        for r in FAR:
            for cp in copies_c(c, r, True):
                cp.start()

    for c in AXES:
        n = TILES[c]
        for r in NEAR:
            for cp in copies_c(c, r, False):
                cp.wait_recv()
        stats = [rst_c[c, i] for i in LINE]
        top, ws, l = weights(stats)
        base = piece(c, 0, 0).start
        for v in range(n):
            o = bc(ws[0], v) * rc[c][0, 8 * v:8 * v + 8, :]
            for i in range(1, 4):
                o = o + bc(ws[i], v) * rc[c][i, 8 * v:8 * v + 8, :]
            o = o / bc(l, 64 + v)
            attn[pl.ds(pl.multiple_of(base + 8 * v, 8), 8), :] = o.astype(BF16).astype(F32)
        for r in FAR:
            copy_gb(c, r, True).start()
        for r in FAR:
            copy_ga(c, r, 0, True).start()

    for q in NEAR:
        for c in AXES:
            copy_gb(c, q, False).wait_recv()
            for r in FAR:
                copy_ga(c, r, q, True).start()

    def t_copy(j):
        return pltpu.make_async_remote_copy(
            src_ref=pout.at[j], dst_ref=pin.at[j], send_sem=t_send.at[j], recv_sem=t_recv.at[j],
            device_id={"tp": 1 - tp}, device_id_type=MESH)

    def out_copy(j):
        cols = pl.ds(j * CW, CW)
        return pltpu.make_async_copy(hid.at[:, cols], out_h.at[:, cols], out_sem.at[j])

    def finish(j):
        cols = pl.ds(j * CW, CW)
        t_copy(j).wait_recv()
        hid[:, cols] = (hid[:, cols].astype(F32) + (pout[j] + pin[j])).astype(BF16)
        out_copy(j).start()

    per = NCHUNK // CUTS
    for i in range(len(ORDER) * CUTS):
        k, cc, slot = i // CUTS, i % CUTS, (i + 5) % SLOTS
        r = ORDER[k]
        if cc == 0:
            if r > 0:
                for c in AXES:
                    for q in (0,) + NEAR:
                        copy_ga(c, r, q, False).wait_recv()
            at = 0
            for c in AXES:
                for h in range(NH[c]):
                    rows = pl.ds(pl.multiple_of((head0(c, r) + h) * BATCH, BATCH), BATCH)
                    lhs[k, :, at:at + HEAD_DIM] = attn[rows, :].astype(BF16)
                    at += HEAD_DIM
        for c in wo_copies(i):
            c.wait()
        for j in range(per * cc, per * cc + per):
            at = (j % per) * CW
            p = jnp.dot(lhs[k], wbuf[slot, :, at:at + CW], preferred_element_type=F32)
            pout[j] = p if k == 0 else pout[j] + p
        if k == CUTS - 1:
            for j in range(per * cc, per * cc + per):
                t_copy(j).start()
            if cc > 0:
                for j in range(per * cc - per, per * cc):
                    finish(j)
        if i + SLOTS < len(ORDER) * CUTS:
            for c in wo_copies(i + SLOTS):
                c.start()
    for j in range(NCHUNK - per, NCHUNK):
        finish(j)

    for g in range(7):
        for r in NEAR:
            q_copy(g, r).wait_send()
    for c in AXES:
        for r in NEAR:
            for g in range(BATCH // BGROUP):
                copy_a(c, r, g).wait_send()
            copy_sa(c, r).wait_send()
            for cp in copies_b(c, r) + copies_c(c, r, True):
                cp.wait_send()
            copy_gb(c, r, True).wait_send()
            for q in LINE:
                copy_ga(c, r, q, True).wait_send()
    c_ko.wait()
    c_vo.wait()

    def drain(j, carry):
        t_copy(j).wait_send()
        out_copy(j).wait()
        return carry
    lax.fori_loop(0, NCHUNK, drain, 0)


def copy_out(*refs):
    n = (len(refs) - 2) // 3
    ins, outs, bufs, i_sem, o_sem = refs[:n], refs[n:2 * n], refs[2 * n:3 * n], refs[-2], refs[-1]
    moves = []
    for k in range(n):
        step = ins[k].shape[0] // BLOCKS
        for j in range(BLOCKS):
            rows = pl.ds(j * step, step)
            moves.append((pltpu.make_async_copy(ins[k].at[rows], bufs[k].at[rows], i_sem.at[k, j]),
                          pltpu.make_async_copy(bufs[k].at[rows], outs[k].at[rows], o_sem.at[k, j])))
    for a, _ in moves:
        a.start()
    for a, b in moves:
        a.wait()
        b.start()
    for _, b in moves:
        b.wait()


def solution(mesh):
    cache_spec = P('dp', 'sp', 'tp', None)

    def local_step(hidden, lengths, k_cache, v_cache, norm_gain, w_query, w_key, w_value, w_out):
        shape = k_cache.shape
        kc = k_cache.reshape(BATCH * SEQ * KV, HEAD_DIM)
        vc = v_cache.reshape(BATCH * SEQ * KV, HEAD_DIM)
        any_ = pl.BlockSpec(memory_space=pl.ANY)
        dma = pltpu.SemaphoreType.DMA
        V = pltpu.VMEM
        n8 = [8 * n for n in TILES]
        rows, half, wide = HEADS * BATCH, D_MODEL // 2, (BATCH, D_MODEL)
        stat = V((3, 4, 8, HEAD_DIM), F32)

        def vec(*lead):
            return [V((*lead, n, HEAD_DIM), F32) for n in n8]

        scratch = [
            V(wide, BF16), V((D_MODEL // HEAD_DIM, HEAD_DIM), BF16), V(wide, BF16), V(kc.shape, BF16), V(vc.shape, BF16),
            V((rows + 2 * KV * BATCH, HEAD_DIM), F32), V((BATCH, HEAD_DIM), jnp.int32),
            V((rows, HEAD_DIM), F32), V((rows, HEAD_DIM), F32),
            stat, *[V((3, n, BATCH, HEAD_DIM), F32) for n in NH], stat, *vec(4), stat, *vec(3), stat, *vec(4), stat,
            V((rows, HEAD_DIM), F32), V((len(ORDER), BATCH, half // len(ORDER)), BF16),
            V((NCHUNK, BATCH, CW), F32), V((NCHUNK, BATCH, CW), F32), V((SLOTS, half // len(ORDER), WIDE), BF16),
            dma((64,)), dma((SLOTS, 3)), dma((NCHUNK,)), dma((2,)),
        ]
        for shape_ in ((7, 3), (3, 3, 5), (3, 3, 2), (3, 3, 2), (3, 3), (3, 3, 4), (NCHUNK,)):
            scratch += [dma(shape_), dma(shape_)]
        res = pl.pallas_call(
            kernel,
            out_shape=(jax.ShapeDtypeStruct((BATCH, D_MODEL), BF16),
                       jax.ShapeDtypeStruct(kc.shape, BF16), jax.ShapeDtypeStruct(vc.shape, BF16)),
            in_specs=[pl.BlockSpec(memory_space=pltpu.SMEM)] + [any_] * 8,
            out_specs=(any_, any_, any_),
            scratch_shapes=scratch,
            compiler_params=pltpu.CompilerParams(
                collective_id=0, has_side_effects=True, vmem_limit_bytes=67043328),
        )(lengths, hidden, norm_gain.reshape(D_MODEL // HEAD_DIM, HEAD_DIM), kc, vc, w_query, w_key, w_value, w_out)
        out, ko, vo = pl.pallas_call(
            copy_out,
            out_shape=tuple(jax.ShapeDtypeStruct(r.shape, r.dtype) for r in res),
            in_specs=[any_] * len(res),
            out_specs=(any_,) * len(res),
            scratch_shapes=[V(r.shape, r.dtype) for r in res] + [dma((len(res), BLOCKS))] * 2,
        )(*res)
        return out, ko.reshape(shape), vo.reshape(shape)

    return jax.shard_map(
        local_step,
        mesh=mesh,
        in_specs=(P('dp', None), P('dp'), cache_spec, cache_spec, P(None), P(None, 'tp'), P(None, 'tp'), P(None, 'tp'), P('tp', None)),
        out_specs=(P('dp', None), cache_spec, cache_spec),
        check_vma=False,
    )
```

```python
import functools

import jax
import jax.numpy as jnp
from jax import lax
from jax.experimental import pallas as pl
from jax.experimental.pallas import tpu as pltpu
from jax.sharding import PartitionSpec as P

EPS = 1e-6
NEG_BIG = -1e30
MESH = pl.DeviceIdType.MESH
F32, BF16 = jnp.float32, jnp.bfloat16

BATCH, D_MODEL, HEAD_DIM = 64, 8192, 128
KV, HEADS, GROUP = 4, 32, 8
SEQ = 16
STRIDE = (1, 4, 16)
FIRST = (0, 12, 24)
NH = (3, 3, 2)
TILES = (6, 6, 4)
SLOTS, CUTS, NCHUNK, CW = 11, 4, 16, 512
WIDE = NCHUNK * CW // CUTS
ORDER = (0, 1, 3, 2)
BGROUP = 16
GROUPS = ((24, 2, 2, 2), (0, 3, 2, 0), (12, 3, 2, 1), (2, 3, 1, 0), (14, 3, 1, 1), (32, 1, 1, 2), (36, 1, 1, 2))
AXES = (0, 1, 2)
LINE = (0, 1, 2, 3)
BLOCKS = 4
NEAR, FAR = (1, 3, 2), (2, 1, 3)


def kernel(lens, hid_h, gain_h, kc_h, vc_h, wq_h, wk_h, wv_h, wo_h,
           out_h, ko_h, vo_h,
           hid, gain, normed, kc, vc, qf, posm, acc, sfull,
           st_a, ra0, ra1, ra2, rst_a,
           b0_, b1_, b2_, rb0, rb1, rb2, rc0, rc1, rc2,
           attn, lhs, pout, pin, wbuf,
           in_sem, w_sem, out_sem, kv_sem, sends,
           q_recv, a_recv, sa_recv, b_recv, c_recv, gb_recv, ga_recv, t_recv):
    sp = lax.axis_index("sp")
    tp = lax.axis_index("tp")
    coord = [sp % 4, (sp // 4) % 4, sp // 16]
    ra, redb, rb, rc = (ra0, ra1, ra2), (b0_, b1_, b2_), (rb0, rb1, rb2), (rc0, rc1, rc2)

    def peer(axis, r):
        c = coord[axis]
        t = (c + r) % 4
        return sp + (t - c) * STRIDE[axis], t

    def remote(src, dst, ss_sem, rs_sem, dev):
        return pltpu.make_async_remote_copy(
            src_ref=src, dst_ref=dst, send_sem=ss_sem, recv_sem=rs_sem,
            device_id={"sp": dev}, device_id_type=MESH)

    def arrived(ref, sem):
        remote(ref, ref, sem, sem, peer(0, 1)[0]).wait_recv()

    c_hid = pltpu.make_async_copy(hid_h, hid, in_sem.at[0])
    c_gain = pltpu.make_async_copy(gain_h, gain, in_sem.at[1])
    c_hid.start()
    c_gain.start()
    x, y, z = coord

    KB = 1024

    def wcols(slot, hbm, col, width, at):
        return [pltpu.make_async_copy(
            hbm.at[pl.ds(k * KB, KB), pl.ds(pl.multiple_of(col, HEAD_DIM), width)],
            wbuf.at[slot, :, pl.ds(k * 256 + at, width)], in_sem.at[2 + slot]) for k in range(D_MODEL // KB)]

    chunks = (
        ((wq_h, 24 + 2 * z),),
        ((wk_h, z), (wv_h, z)),
        ((wq_h, 3 * x),),
        ((wq_h, 12 + 3 * y),),
        ((wq_h, 3 * x + 2), (wq_h, 12 + 3 * y + 2)),
    )
    for i, parts in enumerate(chunks):
        width = 256 // len(parts)
        for k, (hbm, head) in enumerate(parts):
            for c in wcols(i, hbm, head * HEAD_DIM, width, k * width):
                c.start()

    def slot_full(slot, sem):
        pltpu.make_async_copy(wo_h.at[pl.ds(0, KB), pl.ds(0, WIDE)], wbuf.at[slot], sem).wait()

    c_k = pltpu.make_async_copy(kc_h, kc, kv_sem.at[0])
    c_v = pltpu.make_async_copy(vc_h, vc, kv_sem.at[1])

    barrier = pltpu.get_barrier_semaphore()
    for axis in AXES:
        for r in NEAR:
            pl.semaphore_signal(barrier, inc=1, device_id={"sp": peer(axis, r)[0]}, device_id_type=MESH)
    pl.semaphore_signal(barrier, inc=1, device_id={"tp": 1 - tp}, device_id_type=MESH)

    c_hid.wait()
    c_gain.wait()
    ss = jnp.zeros((BATCH, 128), F32)
    for c in range(0, D_MODEL, 512):
        h = hid[:, c:c + 512].astype(F32)
        h = h * h
        ss = ss + ((h[:, 0:128] + h[:, 128:256]) + (h[:, 256:384] + h[:, 384:512]))
    gf = gain[...].astype(F32)
    inv = lax.rsqrt(jnp.sum(ss, axis=1, keepdims=True) * (1.0 / D_MODEL) + EPS)
    for c in range(0, D_MODEL, 512):
        h = hid[:, c:c + 512].astype(F32)
        g = jnp.concatenate([gf[k:k + 1] for k in range(c // HEAD_DIM, (c + 512) // HEAD_DIM)], axis=1)
        normed[:, c:c + 512] = (h * inv * g).astype(BF16)

    def q_copy(g, r):
        base, mult, count, axis = GROUPS[g]
        rows = pl.ds(pl.multiple_of((base + mult * coord[axis]) * BATCH, BATCH), count * BATCH)
        return remote(qf.at[rows], qf.at[rows], sends.at[0], q_recv, peer(axis, r)[0])

    def head0(c, r):
        return FIRST[c] + NH[c] * ((coord[c] + 4 - r) % 4)

    def wo_copies(i):
        slot, r, at, out = (i + 5) % SLOTS, ORDER[i // CUTS], 0, []
        for c in AXES:
            n = NH[c] * HEAD_DIM
            rows = pl.ds(pl.multiple_of(head0(c, r) * HEAD_DIM, HEAD_DIM), n)
            out.append(pltpu.make_async_copy(
                wo_h.at[rows, pl.ds((i % CUTS) * WIDE, WIDE)], wbuf.at[slot, pl.ds(at, n), :], w_sem.at[slot]))
            at += n
        return out

    def put(g, k, val):
        base, mult, count, axis = GROUPS[g]
        rows = pl.ds(pl.multiple_of((base + mult * coord[axis] + k) * BATCH, BATCH), BATCH)
        qf[rows, :] = val.astype(BF16).astype(F32)

    plan = (((0, 0), (0, 1)), ((5, 0), (6, 0)), ((1, 0), (1, 1)), ((2, 0), (2, 1)), ((3, 0), (4, 0)))
    for i in range(5):
        slot_full(i, in_sem.at[2 + i])
        if i == 4:
            c_k.start()
            c_v.start()
            for j in range(6):
                for c in wo_copies(j):
                    c.start()
        res = sum(jnp.dot(normed[:, k * KB:(k + 1) * KB], wbuf[i, :, k * 256:(k + 1) * 256], preferred_element_type=F32)
                  for k in range(D_MODEL // KB))
        (g0, k0), (g1, k1) = plan[i]
        put(g0, k0, res[:, :HEAD_DIM])
        put(g1, k1, res[:, HEAD_DIM:])
        if i == 0:
            pl.semaphore_wait(barrier, 10)
        for g in sorted({g0, g1}):
            for r in FAR:
                q_copy(g, r).start()
    for j in range(6, SLOTS):
        for c in wo_copies(j):
            c.start()

    row = lax.broadcasted_iota(jnp.int32, (64, 128), 0)
    col = lax.broadcasted_iota(jnp.int32, (64, 128), 1)
    own = (row // 32 == col // 64) & ((row % 32) // GROUP == col % KV)
    posm[...] = jnp.where(own, sp * SEQ + (col % 64) // KV, 1 << 30)

    c_k.wait()
    c_v.wait()
    gathered = 3 * (HEADS + 2 * KV) * BATCH // 4
    arrived(qf.at[pl.ds(0, gathered)], q_recv)

    scale = HEAD_DIM ** -0.5
    rpos = sp * SEQ + lax.broadcasted_iota(jnp.int32, (64, 128), 0) // KV
    lane = lax.broadcasted_iota(jnp.int32, (8, 128), 1)
    UN = 4
    acc3 = acc.reshape(HEADS, BATCH, HEAD_DIM)

    def copy_a(c, r, g):
        dev, t = peer(c, r)
        seqs = pl.ds(pl.multiple_of(g * BGROUP, BGROUP), BGROUP)
        return remote(acc3.at[pl.ds(FIRST[c] + NH[c] * t, NH[c]), seqs], ra[c].at[r - 1, :, seqs],
                      sends.at[1], a_recv.at[c], dev)

    def copy_sa(c, r):
        dev, t = peer(c, r)
        return remote(st_a.at[c, t], rst_a.at[c, r - 1], sends.at[2], sa_recv.at[c], dev)

    def attn_part(i):
        lens_, qs, ks, vs = [], [], [], []
        for u in range(UN):
            b = (i * UN + u) * 2
            l0, l1 = lens[b], lens[b + 1]
            lens_.append((l0, l1))
            q = jnp.concatenate([qf[pl.ds(b, 32, stride=64), :], qf[pl.ds(b + 1, 32, stride=64), :]], axis=0)
            qs.append(q.astype(BF16))
            for ref, base, dst in ((kc, 32, ks), (vc, 36, vs)):
                both = []
                for e, ln in ((0, l0), (1, l1)):
                    new = qf[pl.ds(base * 64 + b + e, 4, stride=64), :]
                    new8 = jnp.concatenate([new, new], axis=0)
                    new64 = jnp.concatenate([new8] * 8, axis=0)
                    old = ref[pl.ds(pl.multiple_of((b + e) * 64, 64), 64), :]
                    both.append(jnp.where(rpos == ln, new64, old.astype(F32)).astype(BF16))
                val = jnp.concatenate(both, axis=0)
                ref[pl.ds(pl.multiple_of(b * 64, 128), 128), :] = val
                dst.append(val)
        ss_ = [lax.dot_general(qs[u], ks[u], (((1,), (1,)), ((), ())), preferred_element_type=F32) for u in range(UN)]
        ps, sts = [], []
        for u in range(UN):
            l0, l1 = lens_[u]
            pm = posm[...]
            valid = jnp.concatenate([pm[0:32] <= l0, pm[32:64] <= l1], axis=0)
            s = jnp.where(valid, ss_[u] * scale, NEG_BIG)
            m = jnp.max(s, axis=1, keepdims=True)
            e = jnp.where(valid, jnp.exp(s - m), 0.0)
            l = jnp.sum(e, axis=1, keepdims=True)
            ps.append(e.astype(BF16))
            col2 = lax.broadcasted_iota(jnp.int32, (64, 128), 1)
            sts.append(jnp.where(col2 < 64, m, l))
        for u in range(UN):
            b = (i * UN + u) * 2
            o = jnp.dot(ps[u], vs[u], preferred_element_type=F32)
            acc[pl.ds(b, 32, stride=64), :] = o[0:32]
            acc[pl.ds(b + 1, 32, stride=64), :] = o[32:64]
            sfull[pl.ds(b, 32, stride=64), :] = sts[u][0:32]
            sfull[pl.ds(b + 1, 32, stride=64), :] = sts[u][32:64]

    def attn_body(g, carry):
        per = BGROUP // 2 // UN
        for k in range(per):
            attn_part(g * per + k)
        for r in FAR:
            for c in AXES:
                copy_a(c, r, g).start()
        return carry

    lax.fori_loop(0, BATCH // BGROUP, attn_body, 0)

    c_ko = pltpu.make_async_copy(kc, ko_h, kv_sem.at[0])
    c_vo = pltpu.make_async_copy(vc, vo_h, kv_sem.at[1])
    c_ko.start()
    c_vo.start()

    lane64 = lane % 64
    for c in AXES:
        for a in LINE:
            st = jnp.zeros((8, 128), F32)
            for j in range(8 * NH[c]):
                r0 = (FIRST[c] + NH[c] * a) * BATCH + 8 * j
                st = jnp.where(lane64 == j, sfull[r0:r0 + 8, :], st)
            st_a[c, a] = st

    def copy_b(c, r):
        dev, t = peer((c + 1) % 3, r)
        return remote(redb[c].at[t], rb[c].at[r - 1], sends.at[3], b_recv.at[c], dev)

    def copy_c(c, r):
        axis = (c + 2) % 3
        at = coord[axis]
        return remote(rc[c].at[at], rc[c].at[at], sends.at[4], c_recv.at[c], peer(axis, r)[0])

    def piece(c, ra_, rb_):
        b = (coord[(c + 1) % 3] + 4 - rb_) % 4
        return pl.ds(pl.multiple_of(head0(c, ra_) * BATCH + b * (8 * TILES[c]), 8), 8 * TILES[c])

    def copy_gb(c, r):
        rows = piece(c, 0, 0)
        return remote(attn.at[rows], attn.at[rows], sends.at[5], gb_recv.at[r - 1], peer((c + 1) % 3, r)[0])

    def copy_ga(c, r, q):
        rows = piece(c, 0, q)
        return remote(attn.at[rows], attn.at[rows], sends.at[6], ga_recv.at[r - 1], peer(c, r)[0])

    for r in FAR:
        for c in AXES:
            copy_sa(c, r).start()

    def weights(stats):
        top = functools.reduce(jnp.maximum, stats)
        ws = [jnp.exp(s - top) for s in stats]
        l = sum(pltpu.roll(w, 64, 1) * s for w, s in zip(ws, stats))
        return top, ws, l

    def bc(w, j):
        return jnp.broadcast_to(w[:, j:j + 1], (8, 128))

    for c in AXES:
        n = TILES[c]
        arrived(ra[c], a_recv.at[c])
        arrived(rst_a.at[c], sa_recv.at[c])
        a = coord[c]
        stats = [st_a[c, a]] + [rst_a[c, r] for r in AXES]
        top, ws, l = weights(stats)
        st = jnp.where(lane < 64, top, l)
        for j in range(8 * NH[c]):
            p, v, h, k = j // n, j % n, j // 8, j % 8
            o = bc(ws[0], j) * acc[pl.ds(pl.multiple_of(head0(c, 0) * BATCH + 8 * j, 8), 8), :]
            for r in AXES:
                o = o + bc(ws[r + 1], j) * ra[c][r, h, 8 * k:8 * k + 8, :]
            redb[c][p, 8 * v:8 * v + 8, :] = o
        for p in LINE:
            redb[c][p, 8 * n:, :] = st if p == 0 else pltpu.roll(st, 128 - p * n, 1)
        for r in FAR:
            copy_b(c, r).start()

    for c in AXES:
        n = TILES[c]
        arrived(rb[c], b_recv.at[c])
        b = coord[(c + 1) % 3]
        me = coord[(c + 2) % 3]
        stats = [redb[c][b, 8 * n:, :]] + [rb[c][r, 8 * n:, :] for r in AXES]
        top, ws, l = weights(stats)
        for v in range(n):
            o = bc(ws[0], v) * redb[c][b, 8 * v:8 * v + 8, :]
            for r in AXES:
                o = o + bc(ws[r + 1], v) * rb[c][r, 8 * v:8 * v + 8, :]
            rc[c][me, 8 * v:8 * v + 8, :] = o
        rc[c][me, 8 * n:, :] = jnp.where(lane < 64, top, l)
        for r in FAR:
            copy_c(c, r).start()

    for c in AXES:
        n = TILES[c]
        arrived(rc[c].at[pl.ds(0, 3)], c_recv.at[c])
        stats = [rc[c][i, 8 * n:, :] for i in LINE]
        top, ws, l = weights(stats)
        base = piece(c, 0, 0).start
        for v in range(n):
            o = bc(ws[0], v) * rc[c][0, 8 * v:8 * v + 8, :]
            for i in range(1, 4):
                o = o + bc(ws[i], v) * rc[c][i, 8 * v:8 * v + 8, :]
            o = o / bc(l, 64 + v)
            attn[pl.ds(pl.multiple_of(base + 8 * v, 8), 8), :] = o.astype(BF16).astype(F32)
        for r in FAR:
            copy_gb(c, r).start()
        for r in FAR:
            copy_ga(c, r, 0).start()

    share = HEADS * BATCH // 4
    for q in NEAR:
        arrived(attn.at[pl.ds(0, share // 4)], gb_recv.at[q - 1])
        for c in AXES:
            for r in FAR:
                copy_ga(c, r, q).start()

    per = NCHUNK // CUTS

    def t_copy(cc):
        part = pl.ds(per * cc, per)
        return pltpu.make_async_remote_copy(
            src_ref=pout.at[part], dst_ref=pin.at[part], send_sem=sends.at[7], recv_sem=t_recv.at[cc],
            device_id={"tp": 1 - tp}, device_id_type=MESH)

    def finish(cc):
        t_copy(cc).wait_recv()
        for j in range(per * cc, per * cc + per):
            cols = pl.ds(j * CW, CW)
            hid[:, cols] = (hid[:, cols].astype(F32) + (pout[j] + pin[j])).astype(BF16)
        cols = pl.ds(cc * WIDE, WIDE)
        pltpu.make_async_copy(hid.at[:, cols], out_h.at[:, cols], out_sem).start()

    for i in range(len(ORDER) * CUTS):
        k, cc, slot = i // CUTS, i % CUTS, (i + 5) % SLOTS
        r = ORDER[k]
        if cc == 0:
            if r > 0:
                arrived(attn.at[pl.ds(0, share)], ga_recv.at[r - 1])
            at = 0
            for c in AXES:
                for h in range(NH[c]):
                    rows = pl.ds(pl.multiple_of((head0(c, r) + h) * BATCH, BATCH), BATCH)
                    lhs[k, :, at:at + HEAD_DIM] = attn[rows, :].astype(BF16)
                    at += HEAD_DIM
        slot_full(slot, w_sem.at[slot])
        for j in range(per * cc, per * cc + per):
            at = (j % per) * CW
            p = jnp.dot(lhs[k], wbuf[slot, :, at:at + CW], preferred_element_type=F32)
            pout[j] = p if k == 0 else pout[j] + p
        if k == CUTS - 1:
            t_copy(cc).start()
            if cc > 0:
                finish(cc - 1)
        if i + SLOTS < len(ORDER) * CUTS:
            for c in wo_copies(i + SLOTS):
                c.start()
    finish(CUTS - 1)

    strips = sum(TILES) * 8 + 3 * 8
    for k, n in enumerate((gathered, 3 * share, 9 * 8, 3 * strips, 3 * strips, 3 * share // 4, 3 * share)):
        remote(acc.at[pl.ds(0, n)], acc.at[pl.ds(0, n)], sends.at[k], sends.at[k], peer(0, 1)[0]).wait_send()
    remote(pout, pin, sends.at[7], sends.at[7], peer(0, 1)[0]).wait_send()
    c_ko.wait()
    c_vo.wait()
    pltpu.make_async_copy(hid, out_h, out_sem).wait()


def copy_out(*refs):
    n = (len(refs) - 2) // 3
    ins, outs, bufs, i_sem, o_sem = refs[:n], refs[n:2 * n], refs[2 * n:3 * n], refs[-2], refs[-1]
    moves = []
    for k in range(n):
        step = ins[k].shape[0] // BLOCKS
        for j in range(BLOCKS):
            rows = pl.ds(j * step, step)
            moves.append((pltpu.make_async_copy(ins[k].at[rows], bufs[k].at[rows], i_sem.at[k, j]),
                          pltpu.make_async_copy(bufs[k].at[rows], outs[k].at[rows], o_sem.at[k, j])))
    for a, _ in moves:
        a.start()
    for a, b in moves:
        a.wait()
        b.start()
    for _, b in moves:
        b.wait()


def solution(mesh):
    cache_spec = P('dp', 'sp', 'tp', None)

    def local_step(hidden, lengths, k_cache, v_cache, norm_gain, w_query, w_key, w_value, w_out):
        shape = k_cache.shape
        kc = k_cache.reshape(BATCH * SEQ * KV, HEAD_DIM)
        vc = v_cache.reshape(BATCH * SEQ * KV, HEAD_DIM)
        any_ = pl.BlockSpec(memory_space=pl.ANY)
        dma = pltpu.SemaphoreType.DMA
        V = pltpu.VMEM
        n8 = [8 * n + 8 for n in TILES]
        rows, half, wide = HEADS * BATCH, D_MODEL // 2, (BATCH, D_MODEL)

        def vec(*lead):
            return [V((*lead, n, HEAD_DIM), F32) for n in n8]

        scratch = [
            V(wide, BF16), V((D_MODEL // HEAD_DIM, HEAD_DIM), BF16), V(wide, BF16), V(kc.shape, BF16), V(vc.shape, BF16),
            V((rows + 2 * KV * BATCH, HEAD_DIM), F32), V((BATCH, HEAD_DIM), jnp.int32),
            V((rows, HEAD_DIM), F32), V((rows, HEAD_DIM), F32),
            V((3, 4, 8, HEAD_DIM), F32), *[V((3, n, BATCH, HEAD_DIM), F32) for n in NH], V((3, 3, 8, HEAD_DIM), F32),
            *vec(4), *vec(3), *vec(4),
            V((rows, HEAD_DIM), F32), V((len(ORDER), BATCH, half // len(ORDER)), BF16),
            V((NCHUNK, BATCH, CW), F32), V((NCHUNK, BATCH, CW), F32), V((SLOTS, half // len(ORDER), WIDE), BF16),
            dma((7,)), dma((SLOTS,)), dma, dma((2,)), dma((8,)),
            dma, dma((3,)), dma((3,)), dma((3,)), dma((3,)), dma((3,)), dma((3,)), dma((CUTS,)),
        ]
        res = pl.pallas_call(
            kernel,
            out_shape=(jax.ShapeDtypeStruct((BATCH, D_MODEL), BF16),
                       jax.ShapeDtypeStruct(kc.shape, BF16), jax.ShapeDtypeStruct(vc.shape, BF16)),
            in_specs=[pl.BlockSpec(memory_space=pltpu.SMEM)] + [any_] * 8,
            out_specs=(any_, any_, any_),
            scratch_shapes=scratch,
            compiler_params=pltpu.CompilerParams(
                collective_id=0, has_side_effects=True, vmem_limit_bytes=67043328),
        )(lengths, hidden, norm_gain.reshape(D_MODEL // HEAD_DIM, HEAD_DIM), kc, vc, w_query, w_key, w_value, w_out)
        out, ko, vo = pl.pallas_call(
            copy_out,
            out_shape=tuple(jax.ShapeDtypeStruct(r.shape, r.dtype) for r in res),
            in_specs=[any_] * len(res),
            out_specs=(any_,) * len(res),
            scratch_shapes=[V(r.shape, r.dtype) for r in res] + [dma((len(res), BLOCKS))] * 2,
        )(*res)
        return out, ko.reshape(shape), vo.reshape(shape)

    return jax.shard_map(
        local_step,
        mesh=mesh,
        in_specs=(P('dp', None), P('dp'), cache_spec, cache_spec, P(None), P(None, 'tp'), P(None, 'tp'), P(None, 'tp'), P('tp', None)),
        out_specs=(P('dp', None), cache_spec, cache_spec),
        check_vma=False,
    )
```

```python
import functools

import jax
import jax.numpy as jnp
from jax import lax
from jax.experimental import pallas as pl
from jax.experimental.pallas import tpu as pltpu
from jax.sharding import PartitionSpec as P

EPS = 1e-6
NEG_BIG = -1e30
MESH = pl.DeviceIdType.MESH
F32, BF16 = jnp.float32, jnp.bfloat16

BATCH, D_MODEL, HEAD_DIM = 64, 8192, 128
KV, HEADS, GROUP = 4, 32, 8
SEQ = 16
STRIDE = (1, 4, 16)
FIRST = (0, 12, 24)
NH = (3, 3, 2)
TILES = (6, 6, 4)
SLOTS, CUTS, NCHUNK, CW = 11, 4, 16, 512
WIDE = NCHUNK * CW // CUTS
ORDER = (0, 1, 3, 2)
PIECES = ([(k, cc) for k in (0, 1) for cc in range(CUTS)]
          + [(k, cc) for cc in range(CUTS) for k in (2, 3)])
PAD = 128
BGROUP = 16
GROUPS = ((24, 2, 2, 2), (0, 3, 2, 0), (12, 3, 2, 1), (2, 3, 1, 0), (14, 3, 1, 1), (32, 1, 1, 2), (36, 1, 1, 2))
AXES = (0, 1, 2)
LINE = (0, 1, 2, 3)
BLOCKS = 4
NEAR, FAR = (1, 3, 2), (2, 1, 3)


def kernel(lens, hid_h, gain_h, kc_h, vc_h, wq_h, wk_h, wv_h, wo_h,
           out_h, ko_h, vo_h,
           hid, gain, normed, kc, vc, qf, posm, acc, sfull,
           st_a, ra0, ra1, ra2, rst_a,
           b0_, b1_, b2_, rb0, rb1, rb2, rc0, rc1, rc2,
           attn, lhs, pout, pin, wbuf,
           in_sem, w_sem, out_sem, kv_sem, sends,
           q_recv, a_recv, sa_recv, b_recv, c_recv, gb_recv, ga_recv, t_recv):
    sp = lax.axis_index("sp")
    tp = lax.axis_index("tp")
    coord = [sp % 4, (sp // 4) % 4, sp // 16]
    ra, redb, rb, rc = (ra0, ra1, ra2), (b0_, b1_, b2_), (rb0, rb1, rb2), (rc0, rc1, rc2)

    def peer(axis, r):
        c = coord[axis]
        t = (c + r) % 4
        return sp + (t - c) * STRIDE[axis], t

    def remote(src, dst, ss_sem, rs_sem, dev):
        return pltpu.make_async_remote_copy(
            src_ref=src, dst_ref=dst, send_sem=ss_sem, recv_sem=rs_sem,
            device_id={"sp": dev}, device_id_type=MESH)

    def arrived(ref, sem):
        remote(ref, ref, sem, sem, peer(0, 1)[0]).wait_recv()

    c_hid = pltpu.make_async_copy(hid_h, hid, in_sem.at[0])
    c_gain = pltpu.make_async_copy(gain_h, gain, in_sem.at[1])
    c_hid.start()
    c_gain.start()
    x, y, z = coord

    KB = 1024

    def wcols(slot, hbm, col, width, at):
        return [pltpu.make_async_copy(
            hbm.at[pl.ds(k * KB, KB), pl.ds(pl.multiple_of(col, HEAD_DIM), width)],
            wbuf.at[slot, :, pl.ds(k * 256 + at, width)], in_sem.at[2 + slot]) for k in range(D_MODEL // KB)]

    chunks = (
        ((wq_h, 24 + 2 * z),),
        ((wk_h, z), (wv_h, z)),
        ((wq_h, 3 * x),),
        ((wq_h, 12 + 3 * y),),
        ((wq_h, 3 * x + 2), (wq_h, 12 + 3 * y + 2)),
    )
    for i, parts in enumerate(chunks):
        width = 256 // len(parts)
        for k, (hbm, head) in enumerate(parts):
            for c in wcols(i, hbm, head * HEAD_DIM, width, k * width):
                c.start()

    def slot_full(slot, sem):
        pltpu.make_async_copy(wo_h.at[pl.ds(0, KB), pl.ds(0, WIDE)], wbuf.at[slot, :, pl.ds(0, WIDE)], sem).wait()

    c_k = pltpu.make_async_copy(kc_h, kc, kv_sem.at[0])
    c_v = pltpu.make_async_copy(vc_h, vc, kv_sem.at[1])

    barrier = pltpu.get_barrier_semaphore()
    for axis in AXES:
        for r in NEAR:
            pl.semaphore_signal(barrier, inc=1, device_id={"sp": peer(axis, r)[0]}, device_id_type=MESH)
    pl.semaphore_signal(barrier, inc=1, device_id={"tp": 1 - tp}, device_id_type=MESH)

    c_hid.wait()
    c_gain.wait()
    ss = jnp.zeros((BATCH, 128), F32)
    for c in range(0, D_MODEL, 512):
        h = hid[:, c:c + 512].astype(F32)
        h = h * h
        ss = ss + ((h[:, 0:128] + h[:, 128:256]) + (h[:, 256:384] + h[:, 384:512]))
    gf = gain[...].astype(F32)
    inv = lax.rsqrt(jnp.sum(ss, axis=1, keepdims=True) * (1.0 / D_MODEL) + EPS)
    for c in range(0, D_MODEL, 512):
        h = hid[:, c:c + 512].astype(F32)
        g = jnp.concatenate([gf[k:k + 1] for k in range(c // HEAD_DIM, (c + 512) // HEAD_DIM)], axis=1)
        normed[:, c:c + 512] = (h * inv * g).astype(BF16)

    def q_copy(g, r):
        base, mult, count, axis = GROUPS[g]
        rows = pl.ds(pl.multiple_of((base + mult * coord[axis]) * BATCH, BATCH), count * BATCH)
        return remote(qf.at[rows], qf.at[rows], sends.at[0], q_recv, peer(axis, r)[0])

    def head0(c, r):
        return FIRST[c] + NH[c] * ((coord[c] + 4 - r) % 4)

    def wo_copies(i):
        slot, r, at, out = i % SLOTS, ORDER[PIECES[i][0]], 0, []
        for c in AXES:
            n = NH[c] * HEAD_DIM
            rows = pl.ds(pl.multiple_of(head0(c, r) * HEAD_DIM, HEAD_DIM), n)
            out.append(pltpu.make_async_copy(
                wo_h.at[rows, pl.ds(PIECES[i][1] * WIDE, WIDE)], wbuf.at[slot, pl.ds(at, n), pl.ds(0, WIDE)], w_sem.at[slot]))
            at += n
        return out

    def put(g, k, val):
        base, mult, count, axis = GROUPS[g]
        rows = pl.ds(pl.multiple_of((base + mult * coord[axis] + k) * BATCH, BATCH), BATCH)
        qf[rows, :] = val.astype(BF16).astype(F32)

    plan = (((0, 0), (0, 1)), ((5, 0), (6, 0)), ((1, 0), (1, 1)), ((2, 0), (2, 1)), ((3, 0), (4, 0)))
    for i in range(5):
        slot_full(i, in_sem.at[2 + i])
        if i == 3:
            c_k.start()
            c_v.start()
        res = sum(jnp.dot(normed[:, k * KB:(k + 1) * KB], wbuf[i, :, k * 256:(k + 1) * 256], preferred_element_type=F32)
                  for k in range(D_MODEL // KB))
        (g0, k0), (g1, k1) = plan[i]
        put(g0, k0, res[:, :HEAD_DIM])
        put(g1, k1, res[:, HEAD_DIM:])
        if i == 0:
            pl.semaphore_wait(barrier, 10)
        for g in sorted({g0, g1}):
            for r in FAR:
                q_copy(g, r).start()
    c_k.wait()
    c_v.wait()
    for j in range(SLOTS):
        for c in wo_copies(j):
            c.start()

    row = lax.broadcasted_iota(jnp.int32, (64, 128), 0)
    col = lax.broadcasted_iota(jnp.int32, (64, 128), 1)
    own = (row // 32 == col // 64) & ((row % 32) // GROUP == col % KV)
    posm[...] = jnp.where(own, sp * SEQ + (col % 64) // KV, 1 << 30)

    gathered = 3 * (HEADS + 2 * KV) * BATCH // 4
    arrived(qf.at[pl.ds(0, gathered)], q_recv)

    scale = HEAD_DIM ** -0.5
    rpos = sp * SEQ + lax.broadcasted_iota(jnp.int32, (64, 128), 0) // KV
    lane = lax.broadcasted_iota(jnp.int32, (8, 128), 1)
    UN = 4
    acc3 = acc.reshape(HEADS, BATCH, HEAD_DIM)

    def copy_a(c, r, g):
        dev, t = peer(c, r)
        seqs = pl.ds(pl.multiple_of(g * BGROUP, BGROUP), BGROUP)
        return remote(acc3.at[pl.ds(FIRST[c] + NH[c] * t, NH[c]), seqs], ra[c].at[r - 1, :, seqs],
                      sends.at[1], a_recv.at[c], dev)

    def copy_sa(c, r):
        dev, t = peer(c, r)
        return remote(st_a.at[c, t], rst_a.at[c, r - 1], sends.at[2], sa_recv.at[c], dev)

    def attn_part(i):
        lens_, qs, ks, vs = [], [], [], []
        for u in range(UN):
            b = (i * UN + u) * 2
            l0, l1 = lens[b], lens[b + 1]
            lens_.append((l0, l1))
            q = jnp.concatenate([qf[pl.ds(b, 32, stride=64), :], qf[pl.ds(b + 1, 32, stride=64), :]], axis=0)
            qs.append(q.astype(BF16))
            for ref, base, dst in ((kc, 32, ks), (vc, 36, vs)):
                both = []
                for e, ln in ((0, l0), (1, l1)):
                    new = qf[pl.ds(base * 64 + b + e, 4, stride=64), :]
                    new8 = jnp.concatenate([new, new], axis=0)
                    new64 = jnp.concatenate([new8] * 8, axis=0)
                    old = ref[pl.ds(pl.multiple_of((b + e) * 64, 64), 64), :]
                    both.append(jnp.where(rpos == ln, new64, old.astype(F32)).astype(BF16))
                val = jnp.concatenate(both, axis=0)
                ref[pl.ds(pl.multiple_of(b * 64, 128), 128), :] = val
                dst.append(val)
        ss_ = [lax.dot_general(qs[u], ks[u], (((1,), (1,)), ((), ())), preferred_element_type=F32) for u in range(UN)]
        ps, sts = [], []
        for u in range(UN):
            l0, l1 = lens_[u]
            pm = posm[...]
            valid = jnp.concatenate([pm[0:32] <= l0, pm[32:64] <= l1], axis=0)
            s = jnp.where(valid, ss_[u] * scale, NEG_BIG)
            m = jnp.max(s, axis=1, keepdims=True)
            e = jnp.where(valid, jnp.exp(s - m), 0.0)
            l = jnp.sum(e, axis=1, keepdims=True)
            ps.append(e.astype(BF16))
            col2 = lax.broadcasted_iota(jnp.int32, (64, 128), 1)
            sts.append(jnp.where(col2 < 64, m, l))
        for u in range(UN):
            b = (i * UN + u) * 2
            o = jnp.dot(ps[u], vs[u], preferred_element_type=F32)
            acc[pl.ds(b, 32, stride=64), :] = o[0:32]
            acc[pl.ds(b + 1, 32, stride=64), :] = o[32:64]
            sfull[pl.ds(b, 32, stride=64), :] = sts[u][0:32]
            sfull[pl.ds(b + 1, 32, stride=64), :] = sts[u][32:64]

    def attn_body(g, carry):
        per = BGROUP // 2 // UN
        for k in range(per):
            attn_part(g * per + k)
        for r in FAR:
            for c in AXES:
                copy_a(c, r, g).start()
        return carry

    lax.fori_loop(0, BATCH // BGROUP, attn_body, 0)

    c_ko = pltpu.make_async_copy(kc, ko_h, kv_sem.at[0])
    c_vo = pltpu.make_async_copy(vc, vo_h, kv_sem.at[1])
    c_ko.start()
    c_vo.start()

    lane64 = lane % 64
    for c in AXES:
        for a in LINE:
            st = jnp.zeros((8, 128), F32)
            for j in range(8 * NH[c]):
                r0 = (FIRST[c] + NH[c] * a) * BATCH + 8 * j
                st = jnp.where(lane64 == j, sfull[r0:r0 + 8, :], st)
            st_a[c, a] = st

    def copy_b(c, r):
        dev, t = peer((c + 1) % 3, r)
        return remote(redb[c].at[t], rb[c].at[r - 1], sends.at[3], b_recv.at[c], dev)

    def copy_c(c, r):
        axis = (c + 2) % 3
        at = coord[axis]
        return remote(rc[c].at[at], rc[c].at[at], sends.at[4], c_recv.at[c], peer(axis, r)[0])

    def piece(c, ra_, rb_):
        b = (coord[(c + 1) % 3] + 4 - rb_) % 4
        return pl.ds(pl.multiple_of(head0(c, ra_) * BATCH + b * (8 * TILES[c]), 8), 8 * TILES[c])

    def copy_gb(c, r):
        rows = piece(c, 0, 0)
        return remote(attn.at[rows], attn.at[rows], sends.at[5], gb_recv.at[r - 1], peer((c + 1) % 3, r)[0])

    def copy_ga(c, r, q):
        rows = piece(c, 0, q)
        return remote(attn.at[rows], attn.at[rows], sends.at[6], ga_recv.at[r - 1], peer(c, r)[0])

    for r in FAR:
        for c in AXES:
            copy_sa(c, r).start()

    def weights(stats):
        top = functools.reduce(jnp.maximum, stats)
        ws = [jnp.exp(s - top) for s in stats]
        l = sum(pltpu.roll(w, 64, 1) * s for w, s in zip(ws, stats))
        return top, ws, l

    def bc(w, j):
        return jnp.broadcast_to(w[:, j:j + 1], (8, 128))

    for c in AXES:
        n = TILES[c]
        arrived(ra[c], a_recv.at[c])
        arrived(rst_a.at[c], sa_recv.at[c])
        a = coord[c]
        stats = [st_a[c, a]] + [rst_a[c, r] for r in AXES]
        top, ws, l = weights(stats)
        st = jnp.where(lane < 64, top, l)
        for j in range(8 * NH[c]):
            p, v, h, k = j // n, j % n, j // 8, j % 8
            o = bc(ws[0], j) * acc[pl.ds(pl.multiple_of(head0(c, 0) * BATCH + 8 * j, 8), 8), :]
            for r in AXES:
                o = o + bc(ws[r + 1], j) * ra[c][r, h, 8 * k:8 * k + 8, :]
            redb[c][p, 8 * v:8 * v + 8, :] = o
        for p in LINE:
            redb[c][p, 8 * n:, :] = st if p == 0 else pltpu.roll(st, 128 - p * n, 1)
        for r in FAR:
            copy_b(c, r).start()

    for c in AXES:
        n = TILES[c]
        arrived(rb[c], b_recv.at[c])
        b = coord[(c + 1) % 3]
        me = coord[(c + 2) % 3]
        stats = [redb[c][b, 8 * n:, :]] + [rb[c][r, 8 * n:, :] for r in AXES]
        top, ws, l = weights(stats)
        for v in range(n):
            o = bc(ws[0], v) * redb[c][b, 8 * v:8 * v + 8, :]
            for r in AXES:
                o = o + bc(ws[r + 1], v) * rb[c][r, 8 * v:8 * v + 8, :]
            rc[c][me, 8 * v:8 * v + 8, :] = o
        rc[c][me, 8 * n:, :] = jnp.where(lane < 64, top, l)
        for r in FAR:
            copy_c(c, r).start()

    for c in AXES:
        n = TILES[c]
        arrived(rc[c].at[pl.ds(0, 3)], c_recv.at[c])
        stats = [rc[c][i, 8 * n:, :] for i in LINE]
        top, ws, l = weights(stats)
        base = piece(c, 0, 0).start
        for v in range(n):
            o = bc(ws[0], v) * rc[c][0, 8 * v:8 * v + 8, :]
            for i in range(1, 4):
                o = o + bc(ws[i], v) * rc[c][i, 8 * v:8 * v + 8, :]
            o = o / bc(l, 64 + v)
            attn[pl.ds(pl.multiple_of(base + 8 * v, 8), 8), :] = o.astype(BF16).astype(F32)
        for r in FAR:
            copy_gb(c, r).start()
        for r in FAR:
            copy_ga(c, r, 0).start()

    share = HEADS * BATCH // 4
    for q in NEAR:
        arrived(attn.at[pl.ds(0, share // 4)], gb_recv.at[q - 1])
        for c in AXES:
            for r in FAR:
                copy_ga(c, r, q).start()

    per = NCHUNK // CUTS
    hp = per // 2

    def t_copy(u):
        part = pl.ds(hp * u, hp)
        return pltpu.make_async_remote_copy(
            src_ref=pout.at[part], dst_ref=pin.at[part], send_sem=sends.at[7], recv_sem=t_recv.at[u],
            device_id={"tp": 1 - tp}, device_id_type=MESH)

    def finish(u):
        t_copy(u).wait_recv()
        for j in range(hp * u, hp * u + hp):
            cols = pl.ds(j * CW, CW)
            hid[:, cols] = (hid[:, cols].astype(F32) + (pout[j] + pin[j])).astype(BF16)
        cols = pl.ds(u * hp * CW, hp * CW)
        pltpu.make_async_copy(hid.at[:, cols], out_h.at[:, cols], out_sem).start()

    def take(k):
        r, at = ORDER[k], 0
        if r > 0:
            arrived(attn.at[pl.ds(0, share)], ga_recv.at[r - 1])
        for c in AXES:
            for h in range(NH[c]):
                rows = pl.ds(pl.multiple_of((head0(c, r) + h) * BATCH, BATCH), BATCH)
                lhs[k, :, at:at + HEAD_DIM] = attn[rows, :].astype(BF16)
                at += HEAD_DIM

    def part(i, j):
        at = (j % per) * CW
        return jnp.dot(lhs[PIECES[i][0]], wbuf[i % SLOTS, :, at:at + CW], preferred_element_type=F32)

    for i in range(0, len(PIECES), 2):
        pair = (i, i + 1)
        if i in (0, CUTS):
            take(i // CUTS)
        if i == 2 * CUTS:
            take(2)
            take(3)
        for e in pair:
            slot_full(e % SLOTS, w_sem.at[e % SLOTS])
        if i < 2 * CUTS:
            for e in pair:
                k, cc = PIECES[e]
                for j in range(per * cc, per * cc + per):
                    pout[j] = part(e, j) if k == 0 else pout[j] + part(e, j)
        else:
            cc = PIECES[i][1]
            for u in (2 * cc, 2 * cc + 1):
                for j in range(hp * u, hp * u + hp):
                    pout[j] = pout[j] + (part(i, j) + part(i + 1, j))
                if cc == CUTS - 1:
                    t_copy(u).start()
            if cc < CUTS - 1:
                t_copy(2 * cc).start()
                t_copy(2 * cc + 1).start()
            if cc >= 2:
                finish(2 * cc - 4)
                finish(2 * cc - 3)
        for e in pair:
            if e + SLOTS < len(PIECES):
                for c in wo_copies(e + SLOTS):
                    c.start()
    for u in range(2 * CUTS - 4, 2 * CUTS):
        finish(u)

    strips = sum(TILES) * 8 + 3 * 8
    for k, n in enumerate((gathered, 3 * share, 9 * 8, 3 * strips, 3 * strips, 3 * share // 4, 3 * share)):
        remote(acc.at[pl.ds(0, n)], acc.at[pl.ds(0, n)], sends.at[k], sends.at[k], peer(0, 1)[0]).wait_send()
    remote(pout, pin, sends.at[7], sends.at[7], peer(0, 1)[0]).wait_send()
    c_ko.wait()
    c_vo.wait()
    pltpu.make_async_copy(hid, out_h, out_sem).wait()


def copy_out(*refs):
    n = (len(refs) - 2) // 3
    ins, outs, bufs, i_sem, o_sem = refs[:n], refs[n:2 * n], refs[2 * n:3 * n], refs[-2], refs[-1]
    moves = []
    for k in range(n):
        step = ins[k].shape[0] // BLOCKS
        for j in range(BLOCKS):
            rows = pl.ds(j * step, step)
            moves.append((pltpu.make_async_copy(ins[k].at[rows], bufs[k].at[rows], i_sem.at[k, j]),
                          pltpu.make_async_copy(bufs[k].at[rows], outs[k].at[rows], o_sem.at[k, j])))
    for a, _ in moves:
        a.start()
    for a, b in moves:
        a.wait()
        b.start()
    for _, b in moves:
        b.wait()


def solution(mesh):
    cache_spec = P('dp', 'sp', 'tp', None)

    def local_step(hidden, lengths, k_cache, v_cache, norm_gain, w_query, w_key, w_value, w_out):
        shape = k_cache.shape
        kc = k_cache.reshape(BATCH * SEQ * KV, HEAD_DIM)
        vc = v_cache.reshape(BATCH * SEQ * KV, HEAD_DIM)
        any_ = pl.BlockSpec(memory_space=pl.ANY)
        dma = pltpu.SemaphoreType.DMA
        V = pltpu.VMEM
        n8 = [8 * n + 8 for n in TILES]
        rows, half, wide = HEADS * BATCH, D_MODEL // 2, (BATCH, D_MODEL)

        def vec(*lead):
            return [V((*lead, n, HEAD_DIM), F32) for n in n8]

        scratch = [
            V(wide, BF16), V((D_MODEL // HEAD_DIM, HEAD_DIM), BF16), V(wide, BF16), V(kc.shape, BF16), V(vc.shape, BF16),
            V((rows + 2 * KV * BATCH, HEAD_DIM), F32), V((BATCH, HEAD_DIM), jnp.int32),
            V((rows, HEAD_DIM), F32), V((rows, HEAD_DIM), F32),
            V((3, 4, 8, HEAD_DIM), F32), *[V((3, n, BATCH, HEAD_DIM), F32) for n in NH], V((3, 3, 8, HEAD_DIM), F32),
            *vec(4), *vec(3), *vec(4),
            V((rows, HEAD_DIM), F32), V((len(ORDER), BATCH, half // len(ORDER)), BF16),
            V((NCHUNK, BATCH, CW), F32), V((NCHUNK, BATCH, CW), F32), V((SLOTS, half // len(ORDER), WIDE + PAD), BF16),
            dma((7,)), dma((SLOTS,)), dma, dma((2,)), dma((8,)),
            dma, dma((3,)), dma((3,)), dma((3,)), dma((3,)), dma((3,)), dma((3,)), dma((2 * CUTS,)),
        ]
        res = pl.pallas_call(
            kernel,
            out_shape=(jax.ShapeDtypeStruct((BATCH, D_MODEL), BF16),
                       jax.ShapeDtypeStruct(kc.shape, BF16), jax.ShapeDtypeStruct(vc.shape, BF16)),
            in_specs=[pl.BlockSpec(memory_space=pltpu.SMEM)] + [any_] * 8,
            out_specs=(any_, any_, any_),
            scratch_shapes=scratch,
            compiler_params=pltpu.CompilerParams(
                collective_id=0, has_side_effects=True, vmem_limit_bytes=67043328),
        )(lengths, hidden, norm_gain.reshape(D_MODEL // HEAD_DIM, HEAD_DIM), kc, vc, w_query, w_key, w_value, w_out)
        out, ko, vo = pl.pallas_call(
            copy_out,
            out_shape=tuple(jax.ShapeDtypeStruct(r.shape, r.dtype) for r in res),
            in_specs=[any_] * len(res),
            out_specs=(any_,) * len(res),
            scratch_shapes=[V(r.shape, r.dtype) for r in res] + [dma((len(res), BLOCKS))] * 2,
        )(*res)
        return out, ko.reshape(shape), vo.reshape(shape)

    return jax.shard_map(
        local_step,
        mesh=mesh,
        in_specs=(P('dp', None), P('dp'), cache_spec, cache_spec, P(None), P(None, 'tp'), P(None, 'tp'), P(None, 'tp'), P('tp', None)),
        out_specs=(P('dp', None), cache_spec, cache_spec),
        check_vma=False,
    )
```

```python
import functools

import jax
import jax.numpy as jnp
from jax import lax
from jax.experimental import pallas as pl
from jax.experimental.pallas import tpu as pltpu
from jax.sharding import PartitionSpec as P

EPS = 1e-6
NEG_BIG = -1e30
MESH = pl.DeviceIdType.MESH
F32, BF16 = jnp.float32, jnp.bfloat16

BATCH, D_MODEL, HEAD_DIM = 64, 8192, 128
KV, HEADS, GROUP = 4, 32, 8
SEQ = 16
STRIDE = (1, 4, 16)
FIRST = (0, 12, 24)
NH = (3, 3, 2)
TILES = (6, 6, 4)
SLOTS, CUTS, NCHUNK, CW = 11, 4, 16, 512
WIDE = NCHUNK * CW // CUTS
ORDER = (0, 1, 3, 2)
PIECES = ([(k, cc) for k in (0, 1) for cc in range(CUTS)]
          + [(k, cc) for cc in range(CUTS) for k in (2, 3)])
PITCH = 72
PAD = 128
BGROUP = 16
GROUPS = ((24, 2, 2, 2), (0, 3, 2, 0), (12, 3, 2, 1), (2, 3, 1, 0), (14, 3, 1, 1), (32, 1, 1, 2), (36, 1, 1, 2))
AXES = (0, 1, 2)
LINE = (0, 1, 2, 3)
BLOCKS = 4
NEAR, FAR = (1, 3, 2), (2, 1, 3)


def kernel(lens_h, hid_h, gain_h, kc_h, vc_h, wq_h, wk_h, wv_h, wo_h,
           out_h, ko_h, vo_h,
           lens, hid, gain, normed, kc, vc, qf, posm, acc, sfull,
           st_a, ra0, ra1, ra2, rst_a,
           b0_, b1_, b2_, rb0, rb1, rb2, rc0, rc1, rc2,
           attn, lhs, pout, pin, wbuf,
           in_sem, w_sem, out_sem, kv_sem, sends,
           q_recv, a_recv, sa_recv, b_recv, c_recv, gb_recv, ga_recv, t_recv):
    sp = lax.axis_index("sp")
    tp = lax.axis_index("tp")
    coord = [sp % 4, (sp // 4) % 4, sp // 16]
    ra, redb, rb, rc = (ra0, ra1, ra2), (b0_, b1_, b2_), (rb0, rb1, rb2), (rc0, rc1, rc2)

    def peer(axis, r):
        c = coord[axis]
        t = (c + r) % 4
        return sp + (t - c) * STRIDE[axis], t

    def remote(src, dst, ss_sem, rs_sem, dev):
        return pltpu.make_async_remote_copy(
            src_ref=src, dst_ref=dst, send_sem=ss_sem, recv_sem=rs_sem,
            device_id={"sp": dev}, device_id_type=MESH)

    def arrived(ref, sem):
        remote(ref, ref, sem, sem, peer(0, 1)[0]).wait_recv()

    c_hid = pltpu.make_async_copy(hid_h, hid, in_sem.at[0])
    c_gain = pltpu.make_async_copy(gain_h, gain, in_sem.at[1])
    c_len = pltpu.make_async_copy(lens_h, lens, kv_sem.at[2])
    c_len.start()
    c_hid.start()
    c_gain.start()
    x, y, z = coord

    KB = 1024

    def wcols(slot, hbm, col, width, at):
        return [pltpu.make_async_copy(
            hbm.at[pl.ds(k * KB, KB), pl.ds(pl.multiple_of(col, HEAD_DIM), width)],
            wbuf.at[slot, :, pl.ds(k * 256 + at, width)], in_sem.at[2 + slot]) for k in range(D_MODEL // KB)]

    chunks = (
        ((wq_h, 24 + 2 * z),),
        ((wk_h, z), (wv_h, z)),
        ((wq_h, 3 * x),),
        ((wq_h, 12 + 3 * y),),
        ((wq_h, 3 * x + 2), (wq_h, 12 + 3 * y + 2)),
    )
    for i, parts in enumerate(chunks):
        width = 256 // len(parts)
        for k, (hbm, head) in enumerate(parts):
            for c in wcols(i, hbm, head * HEAD_DIM, width, k * width):
                c.start()

    def slot_full(slot, sem):
        pltpu.make_async_copy(wo_h.at[pl.ds(0, KB), pl.ds(0, WIDE)], wbuf.at[slot, :, pl.ds(0, WIDE)], sem).wait()

    c_k = pltpu.make_async_copy(kc_h, kc, kv_sem.at[0])
    c_v = pltpu.make_async_copy(vc_h, vc, kv_sem.at[1])

    barrier = pltpu.get_barrier_semaphore()
    for axis in AXES:
        for r in NEAR:
            pl.semaphore_signal(barrier, inc=1, device_id={"sp": peer(axis, r)[0]}, device_id_type=MESH)
    pl.semaphore_signal(barrier, inc=1, device_id={"tp": 1 - tp}, device_id_type=MESH)

    c_hid.wait()
    c_gain.wait()
    ss = jnp.zeros((BATCH, 128), F32)
    for c in range(0, D_MODEL, 512):
        h = hid[:, c:c + 512].astype(F32)
        h = h * h
        ss = ss + ((h[:, 0:128] + h[:, 128:256]) + (h[:, 256:384] + h[:, 384:512]))
    gf = gain[...].astype(F32)
    inv = lax.rsqrt(jnp.sum(ss, axis=1, keepdims=True) * (1.0 / D_MODEL) + EPS)
    for c in range(0, D_MODEL, 512):
        h = hid[:, c:c + 512].astype(F32)
        g = jnp.concatenate([gf[k:k + 1] for k in range(c // HEAD_DIM, (c + 512) // HEAD_DIM)], axis=1)
        normed[:, c:c + 512] = (h * inv * g).astype(BF16)

    qf3 = qf.reshape(HEADS + 2 * KV, PITCH, HEAD_DIM)

    def q_copy(g, r):
        base, mult, count, axis = GROUPS[g]
        part = qf3.at[pl.ds(base + mult * coord[axis], count), pl.ds(0, BATCH)]
        return remote(part, part, sends.at[0], q_recv.at[int(base >= HEADS)], peer(axis, r)[0])

    def head0(c, r):
        return FIRST[c] + NH[c] * ((coord[c] + 4 - r) % 4)

    def wo_copies(i):
        slot, r, at, out = i % SLOTS, ORDER[PIECES[i][0]], 0, []
        for c in AXES:
            n = NH[c] * HEAD_DIM
            rows = pl.ds(pl.multiple_of(head0(c, r) * HEAD_DIM, HEAD_DIM), n)
            out.append(pltpu.make_async_copy(
                wo_h.at[rows, pl.ds(PIECES[i][1] * WIDE, WIDE)], wbuf.at[slot, pl.ds(at, n), pl.ds(0, WIDE)], w_sem.at[slot]))
            at += n
        return out

    def put(g, k, val):
        base, mult, count, axis = GROUPS[g]
        rows = pl.ds(pl.multiple_of((base + mult * coord[axis] + k) * PITCH, 8), BATCH)
        qf[rows, :] = val.astype(BF16).astype(F32)

    plan = (((0, 0), (0, 1)), ((5, 0), (6, 0)), ((1, 0), (1, 1)), ((2, 0), (2, 1)), ((3, 0), (4, 0)))
    for i in range(5):
        slot_full(i, in_sem.at[2 + i])
        if i == 3:
            c_k.start()
            c_v.start()
        res = sum(jnp.dot(normed[:, k * KB:(k + 1) * KB], wbuf[i, :, k * 256:(k + 1) * 256], preferred_element_type=F32)
                  for k in range(D_MODEL // KB))
        (g0, k0), (g1, k1) = plan[i]
        put(g0, k0, res[:, :HEAD_DIM])
        put(g1, k1, res[:, HEAD_DIM:])
        if i == 0:
            pl.semaphore_wait(barrier, 10)
        for g in sorted({g0, g1}):
            for r in FAR:
                q_copy(g, r).start()
    c_len.wait()
    c_k.wait()
    c_v.wait()
    for j in range(SLOTS):
        for c in wo_copies(j):
            c.start()

    row = lax.broadcasted_iota(jnp.int32, (64, 128), 0)
    col = lax.broadcasted_iota(jnp.int32, (64, 128), 1)
    own = (row // 32 == col // 64) & ((row % 32) // GROUP == col % KV)
    posm[...] = jnp.where(own, sp * SEQ + (col % 64) // KV, 1 << 30)

    from_q, from_kv = 3 * HEADS * BATCH // 4, 6 * KV * BATCH // 4
    arrived(qf.at[pl.ds(0, from_kv)], q_recv.at[1])
    rpos = sp * SEQ + lax.broadcasted_iota(jnp.int32, (SEQ * KV, HEAD_DIM), 0) // KV

    def place(i, carry):
        for u in range(4):
            b = i * 4 + u
            hit = rpos == lens[b]
            rows = pl.ds(pl.multiple_of(b * SEQ * KV, SEQ * KV), SEQ * KV)
            for ref, base in ((kc, HEADS), (vc, HEADS + KV)):
                new = qf[pl.ds(base * PITCH + b, KV, stride=PITCH), :]
                ref[rows, :] = jnp.where(hit, jnp.concatenate([new] * SEQ, axis=0), ref[rows, :].astype(F32)).astype(BF16)
        return carry

    lax.fori_loop(0, BATCH // 4, place, 0)
    c_ko = pltpu.make_async_copy(kc, ko_h, kv_sem.at[0])
    c_vo = pltpu.make_async_copy(vc, vo_h, kv_sem.at[1])
    c_ko.start()
    c_vo.start()
    arrived(qf.at[pl.ds(0, from_q)], q_recv.at[0])

    scale = HEAD_DIM ** -0.5
    lane = lax.broadcasted_iota(jnp.int32, (8, 128), 1)
    UN = 4
    acc3 = acc.reshape(HEADS, PITCH, HEAD_DIM)

    def copy_a(c, r, g):
        dev, t = peer(c, r)
        seqs = pl.ds(pl.multiple_of(g * BGROUP, BGROUP), BGROUP)
        return remote(acc3.at[pl.ds(FIRST[c] + NH[c] * t, NH[c]), seqs], ra[c].at[r - 1, :, seqs],
                      sends.at[1], a_recv.at[c], dev)

    def copy_sa(c, r):
        dev, t = peer(c, r)
        return remote(st_a.at[c, t], rst_a.at[c, r - 1], sends.at[2], sa_recv.at[c], dev)

    def attn_part(i):
        lens_, qs, ks, vs = [], [], [], []
        for u in range(UN):
            b = (i * UN + u) * 2
            l0, l1 = lens[b], lens[b + 1]
            lens_.append((l0, l1))
            q = jnp.concatenate([qf[pl.ds(b, 32, stride=PITCH), :], qf[pl.ds(b + 1, 32, stride=PITCH), :]], axis=0)
            qs.append(q.astype(BF16))
            rows = pl.ds(pl.multiple_of(b * SEQ * KV, 2 * SEQ * KV), 2 * SEQ * KV)
            ks.append(kc[rows, :])
            vs.append(vc[rows, :])
        ss_ = [lax.dot_general(qs[u], ks[u], (((1,), (1,)), ((), ())), preferred_element_type=F32) for u in range(UN)]
        ps, sts = [], []
        for u in range(UN):
            l0, l1 = lens_[u]
            pm = posm[...]
            valid = jnp.concatenate([pm[0:32] <= l0, pm[32:64] <= l1], axis=0)
            s = jnp.where(valid, ss_[u] * scale, NEG_BIG)
            m = jnp.max(s, axis=1, keepdims=True)
            e = jnp.where(valid, jnp.exp(s - m), 0.0)
            l = jnp.sum(e, axis=1, keepdims=True)
            ps.append(e.astype(BF16))
            col2 = lax.broadcasted_iota(jnp.int32, (64, 128), 1)
            sts.append(jnp.where(col2 < 64, m, l))
        for u in range(UN):
            b = (i * UN + u) * 2
            o = jnp.dot(ps[u], vs[u], preferred_element_type=F32)
            acc[pl.ds(b, 32, stride=PITCH), :] = o[0:32]
            acc[pl.ds(b + 1, 32, stride=PITCH), :] = o[32:64]
            sfull[pl.ds(b, 32, stride=PITCH), :] = sts[u][0:32]
            sfull[pl.ds(b + 1, 32, stride=PITCH), :] = sts[u][32:64]

    def attn_body(g, carry):
        per = BGROUP // 2 // UN
        for k in range(per):
            attn_part(g * per + k)
        for r in FAR:
            for c in AXES:
                copy_a(c, r, g).start()
        return carry

    lax.fori_loop(0, BATCH // BGROUP, attn_body, 0)

    lane64 = lane % 64
    for c in AXES:
        for a in LINE:
            st = jnp.zeros((8, 128), F32)
            for j in range(8 * NH[c]):
                r0 = (FIRST[c] + NH[c] * a + j // 8) * PITCH + 8 * (j % 8)
                st = jnp.where(lane64 == j, sfull[r0:r0 + 8, :], st)
            st_a[c, a] = st

    def copy_b(c, r):
        dev, t = peer((c + 1) % 3, r)
        return remote(redb[c].at[t], rb[c].at[r - 1], sends.at[3], b_recv.at[c], dev)

    def copy_c(c, r):
        axis = (c + 2) % 3
        at = coord[axis]
        return remote(rc[c].at[at], rc[c].at[at], sends.at[4], c_recv.at[c], peer(axis, r)[0])

    def piece(c, ra_, rb_):
        b = (coord[(c + 1) % 3] + 4 - rb_) % 4
        return pl.ds(pl.multiple_of(head0(c, ra_) * BATCH + b * (8 * TILES[c]), 8), 8 * TILES[c])

    def copy_gb(c, r):
        rows = piece(c, 0, 0)
        return remote(attn.at[rows], attn.at[rows], sends.at[5], gb_recv.at[r - 1], peer((c + 1) % 3, r)[0])

    def copy_ga(c, r, q):
        rows = piece(c, 0, q)
        return remote(attn.at[rows], attn.at[rows], sends.at[6], ga_recv.at[r - 1], peer(c, r)[0])

    for r in FAR:
        for c in AXES:
            copy_sa(c, r).start()

    def weights(stats):
        top = functools.reduce(jnp.maximum, stats)
        ws = [jnp.exp(s - top) for s in stats]
        l = sum(pltpu.roll(w, 64, 1) * s for w, s in zip(ws, stats))
        return top, ws, l

    def bc(w, j):
        return jnp.broadcast_to(w[:, j:j + 1], (8, 128))

    for c in AXES:
        n = TILES[c]
        arrived(ra[c], a_recv.at[c])
        arrived(rst_a.at[c], sa_recv.at[c])
        a = coord[c]
        stats = [st_a[c, a]] + [rst_a[c, r] for r in AXES]
        top, ws, l = weights(stats)
        st = jnp.where(lane < 64, top, l)
        for j in range(8 * NH[c]):
            p, v, h, k = j // n, j % n, j // 8, j % 8
            o = bc(ws[0], j) * acc[pl.ds(pl.multiple_of((head0(c, 0) + h) * PITCH + 8 * k, 8), 8), :]
            for r in AXES:
                o = o + bc(ws[r + 1], j) * ra[c][r, h, 8 * k:8 * k + 8, :]
            redb[c][p, 8 * v:8 * v + 8, :] = o
        for p in LINE:
            redb[c][p, 8 * n:, :] = st if p == 0 else pltpu.roll(st, 128 - p * n, 1)
        for r in FAR:
            copy_b(c, r).start()

    for c in AXES:
        n = TILES[c]
        arrived(rb[c], b_recv.at[c])
        b = coord[(c + 1) % 3]
        me = coord[(c + 2) % 3]
        stats = [redb[c][b, 8 * n:, :]] + [rb[c][r, 8 * n:, :] for r in AXES]
        top, ws, l = weights(stats)
        for v in range(n):
            o = bc(ws[0], v) * redb[c][b, 8 * v:8 * v + 8, :]
            for r in AXES:
                o = o + bc(ws[r + 1], v) * rb[c][r, 8 * v:8 * v + 8, :]
            rc[c][me, 8 * v:8 * v + 8, :] = o
        rc[c][me, 8 * n:, :] = jnp.where(lane < 64, top, l)
        for r in FAR:
            copy_c(c, r).start()

    for c in AXES:
        n = TILES[c]
        arrived(rc[c].at[pl.ds(0, 3)], c_recv.at[c])
        stats = [rc[c][i, 8 * n:, :] for i in LINE]
        top, ws, l = weights(stats)
        base = piece(c, 0, 0).start
        for v in range(n):
            o = bc(ws[0], v) * rc[c][0, 8 * v:8 * v + 8, :]
            for i in range(1, 4):
                o = o + bc(ws[i], v) * rc[c][i, 8 * v:8 * v + 8, :]
            o = o / bc(l, 64 + v)
            attn[pl.ds(pl.multiple_of(base + 8 * v, 8), 8), :] = o.astype(BF16).astype(F32)
        for r in FAR:
            copy_gb(c, r).start()
        for r in FAR:
            copy_ga(c, r, 0).start()

    share = HEADS * BATCH // 4
    for q in NEAR:
        arrived(attn.at[pl.ds(0, share // 4)], gb_recv.at[q - 1])
        for c in AXES:
            for r in FAR:
                copy_ga(c, r, q).start()

    per = NCHUNK // CUTS
    hp = per // 2

    def t_copy(u):
        part = pl.ds(hp * u, hp)
        return pltpu.make_async_remote_copy(
            src_ref=pout.at[part], dst_ref=pin.at[part], send_sem=sends.at[7], recv_sem=t_recv.at[u],
            device_id={"tp": 1 - tp}, device_id_type=MESH)

    def finish(u):
        t_copy(u).wait_recv()
        for j in range(hp * u, hp * u + hp):
            cols = pl.ds(j * CW, CW)
            hid[:, cols] = (hid[:, cols].astype(F32) + (pout[j] + pin[j])).astype(BF16)
        cols = pl.ds(u * hp * CW, hp * CW)
        pltpu.make_async_copy(hid.at[:, cols], out_h.at[:, cols], out_sem).start()

    def take(k):
        r, at = ORDER[k], 0
        if r > 0:
            arrived(attn.at[pl.ds(0, share)], ga_recv.at[r - 1])
        for c in AXES:
            for h in range(NH[c]):
                rows = pl.ds(pl.multiple_of((head0(c, r) + h) * BATCH, BATCH), BATCH)
                lhs[k, :, at:at + HEAD_DIM] = attn[rows, :].astype(BF16)
                at += HEAD_DIM

    def part(i, j):
        at = (j % per) * CW
        return jnp.dot(lhs[PIECES[i][0]], wbuf[i % SLOTS, :, at:at + CW], preferred_element_type=F32)

    for i in range(0, len(PIECES), 2):
        pair = (i, i + 1)
        if i in (0, CUTS):
            take(i // CUTS)
        if i == 2 * CUTS:
            take(2)
            take(3)
        for e in pair:
            slot_full(e % SLOTS, w_sem.at[e % SLOTS])
        if i < 2 * CUTS:
            for e in pair:
                k, cc = PIECES[e]
                for j in range(per * cc, per * cc + per):
                    pout[j] = part(e, j) if k == 0 else pout[j] + part(e, j)
        else:
            cc = PIECES[i][1]
            for u in (2 * cc, 2 * cc + 1):
                for j in range(hp * u, hp * u + hp):
                    pout[j] = pout[j] + (part(i, j) + part(i + 1, j))
                if cc == CUTS - 1:
                    t_copy(u).start()
            if cc < CUTS - 1:
                t_copy(2 * cc).start()
                t_copy(2 * cc + 1).start()
            if cc >= 2:
                finish(2 * cc - 4)
                finish(2 * cc - 3)
        for e in pair:
            if e + SLOTS < len(PIECES):
                for c in wo_copies(e + SLOTS):
                    c.start()
    for u in range(2 * CUTS - 4, 2 * CUTS):
        finish(u)

    strips = sum(TILES) * 8 + 3 * 8
    for k, n in enumerate((from_q + from_kv, 3 * share, 9 * 8, 3 * strips, 3 * strips, 3 * share // 4, 3 * share)):
        remote(acc.at[pl.ds(0, n)], acc.at[pl.ds(0, n)], sends.at[k], sends.at[k], peer(0, 1)[0]).wait_send()
    remote(pout, pin, sends.at[7], sends.at[7], peer(0, 1)[0]).wait_send()
    c_ko.wait()
    c_vo.wait()
    pltpu.make_async_copy(hid, out_h, out_sem).wait()


def copy_out(*refs):
    n = (len(refs) - 2) // 3
    ins, outs, bufs, i_sem, o_sem = refs[:n], refs[n:2 * n], refs[2 * n:3 * n], refs[-2], refs[-1]
    moves = []
    for k in range(n):
        step = ins[k].shape[0] // BLOCKS
        for j in range(BLOCKS):
            rows = pl.ds(j * step, step)
            moves.append((pltpu.make_async_copy(ins[k].at[rows], bufs[k].at[rows], i_sem.at[k, j]),
                          pltpu.make_async_copy(bufs[k].at[rows], outs[k].at[rows], o_sem.at[k, j])))
    for a, _ in moves:
        a.start()
    for a, b in moves:
        a.wait()
        b.start()
    for _, b in moves:
        b.wait()


def solution(mesh):
    cache_spec = P('dp', 'sp', 'tp', None)

    def local_step(hidden, lengths, k_cache, v_cache, norm_gain, w_query, w_key, w_value, w_out):
        shape = k_cache.shape
        kc = k_cache.reshape(BATCH * SEQ * KV, HEAD_DIM)
        vc = v_cache.reshape(BATCH * SEQ * KV, HEAD_DIM)
        any_ = pl.BlockSpec(memory_space=pl.ANY)
        dma = pltpu.SemaphoreType.DMA
        V = pltpu.VMEM
        n8 = [8 * n + 8 for n in TILES]
        rows, half, wide = HEADS * BATCH, D_MODEL // 2, (BATCH, D_MODEL)

        def vec(*lead):
            return [V((*lead, n, HEAD_DIM), F32) for n in n8]

        scratch = [
            pltpu.SMEM((BATCH,), jnp.int32), V(wide, BF16), V((D_MODEL // HEAD_DIM, HEAD_DIM), BF16), V(wide, BF16), V(kc.shape, BF16), V(vc.shape, BF16),
            V(((HEADS + 2 * KV) * PITCH, HEAD_DIM), F32), V((BATCH, HEAD_DIM), jnp.int32),
            V((HEADS * PITCH, HEAD_DIM), F32), V((HEADS * PITCH, HEAD_DIM), F32),
            V((3, 4, 8, HEAD_DIM), F32), *[V((3, n, BATCH, HEAD_DIM), F32) for n in NH], V((3, 3, 8, HEAD_DIM), F32),
            *vec(4), *vec(3), *vec(4),
            V((rows, HEAD_DIM), F32), V((len(ORDER), BATCH, half // len(ORDER)), BF16),
            V((NCHUNK, BATCH, CW), F32), V((NCHUNK, BATCH, CW), F32), V((SLOTS, half // len(ORDER), WIDE + PAD), BF16),
            dma((7,)), dma((SLOTS,)), dma, dma((3,)), dma((8,)),
            dma((2,)), *[dma((3,))] * 6, dma((2 * CUTS,)),
        ]
        res = pl.pallas_call(
            kernel,
            out_shape=(jax.ShapeDtypeStruct((BATCH, D_MODEL), BF16),
                       jax.ShapeDtypeStruct(kc.shape, BF16), jax.ShapeDtypeStruct(vc.shape, BF16)),
            in_specs=[any_] * 9,
            out_specs=(any_, any_, any_),
            scratch_shapes=scratch,
            compiler_params=pltpu.CompilerParams(
                collective_id=0, has_side_effects=True, vmem_limit_bytes=67043328),
        )(lengths, hidden, norm_gain.reshape(D_MODEL // HEAD_DIM, HEAD_DIM), kc, vc, w_query, w_key, w_value, w_out)
        out, ko, vo = pl.pallas_call(
            copy_out,
            out_shape=tuple(jax.ShapeDtypeStruct(r.shape, r.dtype) for r in res),
            in_specs=[any_] * len(res),
            out_specs=(any_,) * len(res),
            scratch_shapes=[V(r.shape, r.dtype) for r in res] + [dma((len(res), BLOCKS))] * 2,
        )(*res)
        return out, ko.reshape(shape), vo.reshape(shape)

    return jax.shard_map(
        local_step,
        mesh=mesh,
        in_specs=(P('dp', None), P('dp'), cache_spec, cache_spec, P(None), P(None, 'tp'), P(None, 'tp'), P(None, 'tp'), P('tp', None)),
        out_specs=(P('dp', None), cache_spec, cache_spec),
        check_vma=False,
    )
```

```python
import functools

import jax
import jax.numpy as jnp
from jax import lax
from jax.experimental import pallas as pl
from jax.experimental.pallas import tpu as pltpu
from jax.sharding import PartitionSpec as P

EPS = 1e-6
NEG_BIG = -1e30
MESH = pl.DeviceIdType.MESH
F32, BF16 = jnp.float32, jnp.bfloat16

BATCH, D_MODEL, HEAD_DIM = 64, 8192, 128
KV, HEADS, GROUP = 4, 32, 8
SEQ = 16
STRIDE = (1, 4, 16)
FIRST = (0, 12, 24)
NH = (3, 3, 2)
TILES = (6, 6, 4)
SLOTS, CUTS, NCHUNK, CW = 11, 4, 16, 512
WIDE = NCHUNK * CW // CUTS
ORDER = (0, 1, 3, 2)
PIECES = ([(k, cc) for k in (0, 1) for cc in range(CUTS)]
          + [(k, cc) for cc in range(CUTS) for k in (2, 3)])
PITCH = 72
PAD = 128
BGROUP = 16
GROUPS = ((24, 2, 2, 2), (0, 3, 2, 0), (12, 3, 2, 1), (2, 3, 1, 0), (14, 3, 1, 1), (32, 1, 1, 2), (36, 1, 1, 2))
AXES = (0, 1, 2)
LINE = (0, 1, 2, 3)
BLOCKS = 4
NEAR, FAR = (1, 3, 2), (2, 1, 3)


def kernel(lens_h, hid_h, gain_h, kc_h, vc_h, wq_h, wk_h, wv_h, wo_h,
           out_h, ko_h, vo_h,
           lens, hid, gain, normed, kc, vc, qf, posm, acc, sfull,
           st_a, ra0, ra1, ra2, rst_a,
           b0_, b1_, b2_, rb0, rb1, rb2, rc0, rc1, rc2,
           attn, lhs, pout, pin, wbuf,
           in_sem, w_sem, out_sem, kv_sem, sends,
           q_recv, a_recv, sa_recv, b_recv, c_recv, gb_recv, ga_recv, t_recv):
    sp = lax.axis_index("sp")
    tp = lax.axis_index("tp")
    coord = [sp % 4, (sp // 4) % 4, sp // 16]
    ra, redb, rb, rc = (ra0, ra1, ra2), (b0_, b1_, b2_), (rb0, rb1, rb2), (rc0, rc1, rc2)

    def peer(axis, r):
        c = coord[axis]
        t = (c + r) % 4
        return sp + (t - c) * STRIDE[axis], t

    def remote(src, dst, ss_sem, rs_sem, dev):
        return pltpu.make_async_remote_copy(
            src_ref=src, dst_ref=dst, send_sem=ss_sem, recv_sem=rs_sem,
            device_id={"sp": dev}, device_id_type=MESH)

    def arrived(ref, sem):
        remote(ref, ref, sem, sem, peer(0, 1)[0]).wait_recv()

    c_hid = pltpu.make_async_copy(hid_h, hid, in_sem.at[0])
    c_gain = pltpu.make_async_copy(gain_h, gain, in_sem.at[1])
    c_len = pltpu.make_async_copy(lens_h, lens, kv_sem.at[2])
    c_len.start()
    c_hid.start()
    c_gain.start()
    x, y, z = coord

    KB = 1024

    def wcols(slot, hbm, col, width, at):
        return [pltpu.make_async_copy(
            hbm.at[pl.ds(k * KB, KB), pl.ds(pl.multiple_of(col, HEAD_DIM), width)],
            wbuf.at[slot, :, pl.ds(k * 256 + at, width)], in_sem.at[2 + slot]) for k in range(D_MODEL // KB)]

    chunks = (
        ((wq_h, 24 + 2 * z),),
        ((wk_h, z), (wv_h, z)),
        ((wq_h, 3 * x),),
        ((wq_h, 12 + 3 * y),),
        ((wq_h, 3 * x + 2), (wq_h, 12 + 3 * y + 2)),
    )
    for i, parts in enumerate(chunks):
        width = 256 // len(parts)
        for k, (hbm, head) in enumerate(parts):
            for c in wcols(i, hbm, head * HEAD_DIM, width, k * width):
                c.start()

    def slot_full(slot, sem):
        pltpu.make_async_copy(wo_h.at[pl.ds(0, KB), pl.ds(0, WIDE)], wbuf.at[slot, :, pl.ds(0, WIDE)], sem).wait()

    c_k = pltpu.make_async_copy(kc_h, kc, kv_sem.at[0])
    c_v = pltpu.make_async_copy(vc_h, vc, kv_sem.at[1])

    barrier = pltpu.get_barrier_semaphore()
    for axis in AXES:
        for r in NEAR:
            pl.semaphore_signal(barrier, inc=1, device_id={"sp": peer(axis, r)[0]}, device_id_type=MESH)
    pl.semaphore_signal(barrier, inc=1, device_id={"tp": 1 - tp}, device_id_type=MESH)

    c_hid.wait()
    c_gain.wait()
    ss = jnp.zeros((BATCH, 128), F32)
    for c in range(0, D_MODEL, 512):
        h = hid[:, c:c + 512].astype(F32)
        h = h * h
        ss = ss + ((h[:, 0:128] + h[:, 128:256]) + (h[:, 256:384] + h[:, 384:512]))
    gf = gain[...].astype(F32)
    inv = lax.rsqrt(jnp.sum(ss, axis=1, keepdims=True) * (1.0 / D_MODEL) + EPS)
    for c in range(0, D_MODEL, 512):
        h = hid[:, c:c + 512].astype(F32)
        g = jnp.concatenate([gf[k:k + 1] for k in range(c // HEAD_DIM, (c + 512) // HEAD_DIM)], axis=1)
        normed[:, c:c + 512] = (h * inv * g).astype(BF16)

    qf3 = qf.reshape(HEADS + 2 * KV, PITCH, HEAD_DIM)

    def q_copy(g, r):
        base, mult, count, axis = GROUPS[g]
        part = qf3.at[pl.ds(base + mult * coord[axis], count), pl.ds(0, BATCH)]
        return remote(part, part, sends.at[0], q_recv.at[int(base >= HEADS)], peer(axis, r)[0])

    def head0(c, r):
        return FIRST[c] + NH[c] * ((coord[c] + 4 - r) % 4)

    def wo_copies(i):
        slot, r, at, out = i % SLOTS, ORDER[PIECES[i][0]], 0, []
        for c in AXES:
            n = NH[c] * HEAD_DIM
            rows = pl.ds(pl.multiple_of(head0(c, r) * HEAD_DIM, HEAD_DIM), n)
            out.append(pltpu.make_async_copy(
                wo_h.at[rows, pl.ds(PIECES[i][1] * WIDE, WIDE)], wbuf.at[slot, pl.ds(at, n), pl.ds(0, WIDE)], w_sem.at[slot]))
            at += n
        return out

    def put(g, k, val):
        base, mult, count, axis = GROUPS[g]
        rows = pl.ds(pl.multiple_of((base + mult * coord[axis] + k) * PITCH, 8), BATCH)
        qf[rows, :] = val.astype(BF16).astype(F32)

    plan = (((0, 0), (0, 1)), ((5, 0), (6, 0)), ((1, 0), (1, 1)), ((2, 0), (2, 1)), ((3, 0), (4, 0)))
    for i in range(5):
        slot_full(i, in_sem.at[2 + i])
        if i == 3:
            c_k.start()
            c_v.start()
        res = sum(jnp.dot(normed[:, k * KB:(k + 1) * KB], wbuf[i, :, k * 256:(k + 1) * 256], preferred_element_type=F32)
                  for k in range(D_MODEL // KB))
        (g0, k0), (g1, k1) = plan[i]
        put(g0, k0, res[:, :HEAD_DIM])
        put(g1, k1, res[:, HEAD_DIM:])
        if i == 0:
            pl.semaphore_wait(barrier, 10)
        for g in sorted({g0, g1}):
            for r in FAR:
                q_copy(g, r).start()
    c_len.wait()
    c_k.wait()
    c_v.wait()
    for j in range(SLOTS):
        for c in wo_copies(j):
            c.start()

    row = lax.broadcasted_iota(jnp.int32, (64, 128), 0)
    col = lax.broadcasted_iota(jnp.int32, (64, 128), 1)
    own = (row // 32 == col // 64) & ((row % 32) // GROUP == col % KV)
    posm[...] = jnp.where(own, sp * SEQ + (col % 64) // KV, 1 << 30)

    from_q, from_kv = 3 * HEADS * BATCH // 4, 6 * KV * BATCH // 4
    arrived(qf.at[pl.ds(0, from_kv)], q_recv.at[1])
    rpos = sp * SEQ + lax.broadcasted_iota(jnp.int32, (SEQ * KV, HEAD_DIM), 0) // KV

    def place(i, carry):
        for u in range(4):
            b = i * 4 + u
            hit = rpos == lens[b]
            rows = pl.ds(pl.multiple_of(b * SEQ * KV, SEQ * KV), SEQ * KV)
            for ref, base in ((kc, HEADS), (vc, HEADS + KV)):
                new = qf[pl.ds(base * PITCH + b, KV, stride=PITCH), :]
                ref[rows, :] = jnp.where(hit, jnp.concatenate([new] * SEQ, axis=0), ref[rows, :].astype(F32)).astype(BF16)
        return carry

    lax.fori_loop(0, BATCH // 4, place, 0)
    c_ko = pltpu.make_async_copy(kc, ko_h, kv_sem.at[0])
    c_vo = pltpu.make_async_copy(vc, vo_h, kv_sem.at[1])
    c_ko.start()
    c_vo.start()
    arrived(qf.at[pl.ds(0, from_q)], q_recv.at[0])

    scale = HEAD_DIM ** -0.5
    lane = lax.broadcasted_iota(jnp.int32, (8, 128), 1)
    UN = 4
    acc3 = acc.reshape(HEADS, PITCH, HEAD_DIM)

    def copy_a(c, r, g):
        dev, t = peer(c, r)
        seqs = pl.ds(pl.multiple_of(g * BGROUP, BGROUP), BGROUP)
        return remote(acc3.at[pl.ds(FIRST[c] + NH[c] * t, NH[c]), seqs], ra[c].at[r - 1, :, seqs],
                      sends.at[1], a_recv.at[c], dev)

    def copy_sa(c, r):
        dev, t = peer(c, r)
        return remote(st_a.at[c, t], rst_a.at[c, r - 1], sends.at[2], sa_recv.at[c], dev)

    def attn_part(i):
        lens_, qs, ks, vs = [], [], [], []
        for u in range(UN):
            b = (i * UN + u) * 2
            l0, l1 = lens[b], lens[b + 1]
            lens_.append((l0, l1))
            q = jnp.concatenate([qf[pl.ds(b, 32, stride=PITCH), :], qf[pl.ds(b + 1, 32, stride=PITCH), :]], axis=0)
            qs.append(q.astype(BF16))
            rows = pl.ds(pl.multiple_of(b * SEQ * KV, 2 * SEQ * KV), 2 * SEQ * KV)
            ks.append(kc[rows, :])
            vs.append(vc[rows, :])
        ss_ = [lax.dot_general(qs[u], ks[u], (((1,), (1,)), ((), ())), preferred_element_type=F32) for u in range(UN)]
        ps, sts = [], []
        for u in range(UN):
            l0, l1 = lens_[u]
            pm = posm[...]
            valid = jnp.concatenate([pm[0:32] <= l0, pm[32:64] <= l1], axis=0)
            s = jnp.where(valid, ss_[u] * scale, NEG_BIG)
            m = jnp.max(s, axis=1, keepdims=True)
            e = jnp.where(valid, jnp.exp(s - m), 0.0)
            l = jnp.sum(e, axis=1, keepdims=True)
            ps.append(e.astype(BF16))
            col2 = lax.broadcasted_iota(jnp.int32, (64, 128), 1)
            sts.append(jnp.where(col2 < 64, m, l))
        for u in range(UN):
            b = (i * UN + u) * 2
            o = jnp.dot(ps[u], vs[u], preferred_element_type=F32)
            acc[pl.ds(b, 32, stride=PITCH), :] = o[0:32]
            acc[pl.ds(b + 1, 32, stride=PITCH), :] = o[32:64]
            sfull[pl.ds(b, 32, stride=PITCH), :] = sts[u][0:32]
            sfull[pl.ds(b + 1, 32, stride=PITCH), :] = sts[u][32:64]

    def attn_body(g, carry):
        per = BGROUP // 2 // UN
        for k in range(per):
            attn_part(g * per + k)
        for r in FAR:
            for c in AXES:
                copy_a(c, r, g).start()
        return carry

    lax.fori_loop(0, BATCH // BGROUP, attn_body, 0)

    lane64 = lane % 64
    for c in AXES:
        for a in LINE:
            st = jnp.zeros((8, 128), F32)
            for j in range(8 * NH[c]):
                r0 = (FIRST[c] + NH[c] * a + j // 8) * PITCH + 8 * (j % 8)
                st = jnp.where(lane64 == j, sfull[r0:r0 + 8, :], st)
            st_a[c, a] = st

    def copy_b(c, r):
        dev, t = peer((c + 1) % 3, r)
        return remote(redb[c].at[t], rb[c].at[r - 1], sends.at[3], b_recv.at[c], dev)

    def copy_c(c, r):
        axis = (c + 2) % 3
        at = coord[axis]
        return remote(rc[c].at[at], rc[c].at[at], sends.at[4], c_recv.at[c], peer(axis, r)[0])

    def piece(c, ra_, rb_):
        b = (coord[(c + 1) % 3] + 4 - rb_) % 4
        return pl.ds(pl.multiple_of(head0(c, ra_) * BATCH + b * (8 * TILES[c]), 8), 8 * TILES[c])

    def copy_gb(c, r):
        rows = piece(c, 0, 0)
        return remote(attn.at[rows], attn.at[rows], sends.at[5], gb_recv.at[r - 1], peer((c + 1) % 3, r)[0])

    def copy_ga(c, r, q):
        rows = piece(c, 0, q)
        return remote(attn.at[rows], attn.at[rows], sends.at[6], ga_recv.at[r - 1], peer(c, r)[0])

    for r in FAR:
        for c in AXES:
            copy_sa(c, r).start()

    def weights(stats):
        top = functools.reduce(jnp.maximum, stats)
        ws = [jnp.exp(s - top) for s in stats]
        l = sum(pltpu.roll(w, 64, 1) * s for w, s in zip(ws, stats))
        return top, ws, l

    def bc(w, j):
        return jnp.broadcast_to(w[:, j:j + 1], (8, 128))

    for c in AXES:
        n = TILES[c]
        arrived(ra[c], a_recv.at[c])
        arrived(rst_a.at[c], sa_recv.at[c])
        a = coord[c]
        stats = [st_a[c, a]] + [rst_a[c, r] for r in AXES]
        top, ws, l = weights(stats)
        st = jnp.where(lane < 64, top, l)
        for j in range(8 * NH[c]):
            p, v, h, k = j // n, j % n, j // 8, j % 8
            o = bc(ws[0], j) * acc[pl.ds(pl.multiple_of((head0(c, 0) + h) * PITCH + 8 * k, 8), 8), :]
            for r in AXES:
                o = o + bc(ws[r + 1], j) * ra[c][r, h, 8 * k:8 * k + 8, :]
            redb[c][p, 8 * v:8 * v + 8, :] = o
        for p in LINE:
            redb[c][p, 8 * n:, :] = st if p == 0 else pltpu.roll(st, 128 - p * n, 1)
        for r in FAR:
            copy_b(c, r).start()

    for c in AXES:
        n = TILES[c]
        arrived(rb[c], b_recv.at[c])
        b = coord[(c + 1) % 3]
        me = coord[(c + 2) % 3]
        stats = [redb[c][b, 8 * n:, :]] + [rb[c][r, 8 * n:, :] for r in AXES]
        top, ws, l = weights(stats)
        for v in range(n):
            o = bc(ws[0], v) * redb[c][b, 8 * v:8 * v + 8, :]
            for r in AXES:
                o = o + bc(ws[r + 1], v) * rb[c][r, 8 * v:8 * v + 8, :]
            rc[c][me, 8 * v:8 * v + 8, :] = o
        rc[c][me, 8 * n:, :] = jnp.where(lane < 64, top, l)
        for r in FAR:
            copy_c(c, r).start()

    for c in AXES:
        n = TILES[c]
        arrived(rc[c].at[pl.ds(0, 3)], c_recv.at[c])
        stats = [rc[c][i, 8 * n:, :] for i in LINE]
        top, ws, l = weights(stats)
        base = piece(c, 0, 0).start
        for v in range(n):
            o = bc(ws[0], v) * rc[c][0, 8 * v:8 * v + 8, :]
            for i in range(1, 4):
                o = o + bc(ws[i], v) * rc[c][i, 8 * v:8 * v + 8, :]
            o = o / bc(l, 64 + v)
            attn[pl.ds(pl.multiple_of(base + 8 * v, 8), 8), :] = o.astype(BF16).astype(F32)
        for r in FAR:
            copy_gb(c, r).start()
        for r in NEAR:
            copy_ga(c, r, 0).start()

    share = HEADS * BATCH // 4
    for q in NEAR:
        arrived(attn.at[pl.ds(0, share // 4)], gb_recv.at[q - 1])
        for r in NEAR:
            for c in AXES:
                copy_ga(c, r, q).start()

    per = NCHUNK // CUTS
    hp = per // 2

    def t_copy(u):
        part = pl.ds(hp * u, hp)
        return pltpu.make_async_remote_copy(
            src_ref=pout.at[part], dst_ref=pin.at[part], send_sem=sends.at[7], recv_sem=t_recv.at[u],
            device_id={"tp": 1 - tp}, device_id_type=MESH)

    def finish(u):
        t_copy(u).wait_recv()
        for j in range(hp * u, hp * u + hp):
            cols = pl.ds(j * CW, CW)
            hid[:, cols] = (hid[:, cols].astype(F32) + (pout[j] + pin[j])).astype(BF16)
        cols = pl.ds(u * hp * CW, hp * CW)
        pltpu.make_async_copy(hid.at[:, cols], out_h.at[:, cols], out_sem).start()

    def take(k):
        r, at = ORDER[k], 0
        if r > 0:
            arrived(attn.at[pl.ds(0, share)], ga_recv.at[r - 1])
        for c in AXES:
            for h in range(NH[c]):
                rows = pl.ds(pl.multiple_of((head0(c, r) + h) * BATCH, BATCH), BATCH)
                lhs[k, :, at:at + HEAD_DIM] = attn[rows, :].astype(BF16)
                at += HEAD_DIM

    def part(i, j):
        at = (j % per) * CW
        return jnp.dot(lhs[PIECES[i][0]], wbuf[i % SLOTS, :, at:at + CW], preferred_element_type=F32)

    for i in range(0, len(PIECES), 2):
        pair = (i, i + 1)
        if i in (0, CUTS):
            take(i // CUTS)
        if i == 2 * CUTS:
            take(2)
            take(3)
        for e in pair:
            slot_full(e % SLOTS, w_sem.at[e % SLOTS])
        if i < 2 * CUTS:
            for e in pair:
                k, cc = PIECES[e]
                for j in range(per * cc, per * cc + per):
                    pout[j] = part(e, j) if k == 0 else pout[j] + part(e, j)
        else:
            cc = PIECES[i][1]
            for u in (2 * cc, 2 * cc + 1):
                for j in range(hp * u, hp * u + hp):
                    pout[j] = pout[j] + (part(i, j) + part(i + 1, j))
                if cc == CUTS - 1:
                    t_copy(u).start()
            if cc < CUTS - 1:
                t_copy(2 * cc).start()
                t_copy(2 * cc + 1).start()
            if cc >= 2:
                finish(2 * cc - 4)
                finish(2 * cc - 3)
        for e in pair:
            if e + SLOTS < len(PIECES):
                for c in wo_copies(e + SLOTS):
                    c.start()
    for u in range(2 * CUTS - 4, 2 * CUTS):
        finish(u)

    strips = sum(TILES) * 8 + 3 * 8
    for k, n in enumerate((from_q + from_kv, 3 * share, 9 * 8, 3 * strips, 3 * strips, 3 * share // 4, 3 * share)):
        remote(acc.at[pl.ds(0, n)], acc.at[pl.ds(0, n)], sends.at[k], sends.at[k], peer(0, 1)[0]).wait_send()
    remote(pout, pin, sends.at[7], sends.at[7], peer(0, 1)[0]).wait_send()
    c_ko.wait()
    c_vo.wait()
    pltpu.make_async_copy(hid, out_h, out_sem).wait()


def copy_out(*refs):
    n = (len(refs) - 2) // 3
    ins, outs, bufs, i_sem, o_sem = refs[:n], refs[n:2 * n], refs[2 * n:3 * n], refs[-2], refs[-1]
    moves = []
    for k in range(n):
        step = ins[k].shape[0] // BLOCKS
        for j in range(BLOCKS):
            rows = pl.ds(j * step, step)
            moves.append((pltpu.make_async_copy(ins[k].at[rows], bufs[k].at[rows], i_sem.at[k, j]),
                          pltpu.make_async_copy(bufs[k].at[rows], outs[k].at[rows], o_sem.at[k, j])))
    for a, _ in moves:
        a.start()
    for a, b in moves:
        a.wait()
        b.start()
    for _, b in moves:
        b.wait()


def solution(mesh):
    cache_spec = P('dp', 'sp', 'tp', None)

    def local_step(hidden, lengths, k_cache, v_cache, norm_gain, w_query, w_key, w_value, w_out):
        shape = k_cache.shape
        kc = k_cache.reshape(BATCH * SEQ * KV, HEAD_DIM)
        vc = v_cache.reshape(BATCH * SEQ * KV, HEAD_DIM)
        any_ = pl.BlockSpec(memory_space=pl.ANY)
        dma = pltpu.SemaphoreType.DMA
        V = pltpu.VMEM
        n8 = [8 * n + 8 for n in TILES]
        rows, half, wide = HEADS * BATCH, D_MODEL // 2, (BATCH, D_MODEL)

        def vec(*lead):
            return [V((*lead, n, HEAD_DIM), F32) for n in n8]

        scratch = [
            pltpu.SMEM((BATCH,), jnp.int32), V(wide, BF16), V((D_MODEL // HEAD_DIM, HEAD_DIM), BF16), V(wide, BF16), V(kc.shape, BF16), V(vc.shape, BF16),
            V(((HEADS + 2 * KV) * PITCH, HEAD_DIM), F32), V((BATCH, HEAD_DIM), jnp.int32),
            V((HEADS * PITCH, HEAD_DIM), F32), V((HEADS * PITCH, HEAD_DIM), F32),
            V((3, 4, 8, HEAD_DIM), F32), *[V((3, n, BATCH, HEAD_DIM), F32) for n in NH], V((3, 3, 8, HEAD_DIM), F32),
            *vec(4), *vec(3), *vec(4),
            V((rows, HEAD_DIM), F32), V((len(ORDER), BATCH, half // len(ORDER)), BF16),
            V((NCHUNK, BATCH, CW), F32), V((NCHUNK, BATCH, CW), F32), V((SLOTS, half // len(ORDER), WIDE + PAD), BF16),
            dma((7,)), dma((SLOTS,)), dma, dma((3,)), dma((8,)),
            dma((2,)), *[dma((3,))] * 6, dma((2 * CUTS,)),
        ]
        res = pl.pallas_call(
            kernel,
            out_shape=(jax.ShapeDtypeStruct((BATCH, D_MODEL), BF16),
                       jax.ShapeDtypeStruct(kc.shape, BF16), jax.ShapeDtypeStruct(vc.shape, BF16)),
            in_specs=[any_] * 9,
            out_specs=(any_, any_, any_),
            scratch_shapes=scratch,
            compiler_params=pltpu.CompilerParams(
                collective_id=0, has_side_effects=True, vmem_limit_bytes=67043328),
        )(lengths, hidden, norm_gain.reshape(D_MODEL // HEAD_DIM, HEAD_DIM), kc, vc, w_query, w_key, w_value, w_out)
        out, ko, vo = pl.pallas_call(
            copy_out,
            out_shape=tuple(jax.ShapeDtypeStruct(r.shape, r.dtype) for r in res),
            in_specs=[any_] * len(res),
            out_specs=(any_,) * len(res),
            scratch_shapes=[V(r.shape, r.dtype) for r in res] + [dma((len(res), BLOCKS))] * 2,
        )(*res)
        return out, ko.reshape(shape), vo.reshape(shape)

    return jax.shard_map(
        local_step,
        mesh=mesh,
        in_specs=(P('dp', None), P('dp'), cache_spec, cache_spec, P(None), P(None, 'tp'), P(None, 'tp'), P(None, 'tp'), P('tp', None)),
        out_specs=(P('dp', None), cache_spec, cache_spec),
        check_vma=False,
    )
```
